32 devices in a mesh: comp: 2 (over x), gy: 4 (over z), gx: 4 (over y, core).
Axes of the slice: x: 2, y: 2, z: 4, core: 2. Of those that a mesh axis runs over, the one named last changes fastest.
Arguments:
- column_water: float32 [2, 16, 32, 512], P('comp', None, 'gy', 'gx'), may hold values from 0.2 to 2
- land_soil: float32 [2, 32, 512], P('comp', 'gy', 'gx'), may hold values from 0.1 to 0.9
- level_weight: float32 [16], replicated, may hold values from 0.01 to 0.1
- excess_weight: float32 [16], replicated, may hold values from 0.3 to 3
- soil_weight: float32 [16], replicated, may hold values from 0.3 to 3
- terrain_class: int32 [320, 5120], P('gy', 'gx'), may hold values from 0 to 15
- surface_head: float32 [2, 320, 5120], P('comp', 'gy', 'gx'), may hold values from 0 to 1
- conductivity: float32 [2, 320, 5120], P('comp', 'gy', 'gx'), may hold values from 0.02 to 0.22
- active_mask: int32 [2, 320, 5120], P('comp', 'gy', 'gx'), may hold values 0 or 1
- flow_code: int32 [2, 320, 5120], P('comp', 'gy', 'gx'), may hold values from 0 to 3
Outputs:
- coupled_state: float32 [2, 32, 512], P('comp', 'gy', 'gx')
The draws below stay inside these ranges and needn't reach their ends.
All inputs are finite; a program needn't handle non-finite values. No bound on the sum of `active_mask` on one device may be relied on, other than what follows from the above.
Results may differ from the reference program's by a relative error of at most 0.0003.
Values sent between devices are 32-bit elements; how exact they have to be, the bound alone decides.
A program may use at most 64 MiB of HBM per device.

```python
import math
import jax
import jax.numpy as jnp
from jax import lax

LEV = 16
AGG = 10
NW = 16
NSUB = 8
SWEEPS = 2
NYC = 32
NXC = 512
NYF = 320
NXF = 5120


def with_ends(values, stream_key, smallest, largest):
    dims = values.shape
    place = [jax.random.randint(jax.random.fold_in(stream_key, axis), (), 0, dims[axis]) for axis in range(len(dims))]
    values = values.at[tuple(place)].set(smallest)
    longest = dims.index(max(dims))
    place[longest] = (place[longest] + 1) % dims[longest]
    return values.at[tuple(place)].set(largest)


def levels(stream_key, extent, shards, smallest, high):
    gain, own = 1.0, jax.random.fold_in(stream_key, 6)
    for axis_at, parts in shards:
        steps = jnp.exp(jax.random.uniform(jax.random.fold_in(own, axis_at), (parts,), jnp.float32, smallest / len(shards), high / len(shards)))
        gain = gain * jnp.repeat(steps, extent[axis_at] // parts).reshape([-1 if axis == axis_at else 1 for axis in range(len(extent))])
    return gain


def setup_inputs(seed: int = 0) -> dict:
    key_list = jax.random.split(jax.random.key(seed), 11)
    return {
        "column_water": jnp.clip(jnp.exp(math.log(2.0) - 2.3025851 * jax.random.uniform(key_list[0], (2, LEV, NYC, NXC), jnp.float32) ** levels(key_list[0], (2, LEV, NYC, NXC), ((0, 2), (2, 4), (3, 4)), -0.2, 0.2)), 0.2, 2.0),
        "land_soil": jnp.clip(0.1 + 0.79999997 * jax.random.uniform(key_list[1], (2, NYC, NXC), jnp.float32) ** levels(key_list[1], (2, NYC, NXC), ((0, 2), (1, 4), (2, 4)), -0.2, 0.2), 0.1, 0.9),
        "level_weight": jnp.clip(jnp.exp(jax.random.uniform(key_list[2], (LEV,), jnp.float32, math.log(0.01), math.log(0.1))), 0.01, 0.1),
        "excess_weight": jnp.clip(jnp.exp(jax.random.uniform(key_list[3], (NW,), jnp.float32, math.log(0.3), math.log(3.0))), 0.3, 3.0),
        "soil_weight": jnp.clip(jnp.exp(jax.random.uniform(key_list[4], (NW,), jnp.float32, math.log(0.3), math.log(3.0))), 0.3, 3.0),
        "terrain_class": with_ends(jax.random.randint(key_list[5], (NYF, NXF), 0, NW), jax.random.fold_in(key_list[5], 1), 0, NW - 1).astype(jnp.int32),
        "surface_head": jnp.clip(1.0 * jax.random.uniform(key_list[6], (2, NYF, NXF), jnp.float32) ** levels(key_list[6], (2, NYF, NXF), ((0, 2), (1, 4), (2, 4)), -0.2, 0.2), 0.0, 1.0),
        "conductivity": jnp.clip(jnp.exp(math.log(0.22) - 2.3978953 * jax.random.uniform(key_list[7], (2, NYF, NXF), jnp.float32) ** levels(key_list[7], (2, NYF, NXF), ((0, 2), (1, 4), (2, 4)), -0.2, 0.2)), 0.02, 0.22),
        "active_mask": with_ends((jax.random.randint(key_list[8], (2, NYF, NXF), 0, 10) < 9).astype(jnp.int32), jax.random.fold_in(key_list[8], 1), 0, 1),
        "flow_code": with_ends(jax.random.randint(key_list[9], (2, NYF, NXF), 0, 4), jax.random.fold_in(key_list[9], 1), 0, 3).astype(jnp.int32),
    }


diffusion_rate = 0.2
infiltration_rate = 0.05
drainage_rate = 0.1
half_point = 0.1
evaporation_scale = 0.5

def neighbours(field):
    return (field[:-2, 1:-1], field[2:, 1:-1], field[1:-1, :-2], field[1:-1, 2:])

def lookup(table, classes):
    summed = jnp.zeros(classes.shape, table.dtype)
    for number in range(table.shape[0]):
        summed = summed + jnp.where(classes == number, table[number], 0.0)
    return summed

def block_mean(field):
    rows, cols = field.shape
    return field.reshape(rows // AGG, AGG, cols // AGG, AGG).mean(axis=(1, 3))

def upsample(field):
    return jnp.repeat(jnp.repeat(field, AGG, axis=0), AGG, axis=1)

def disaggregate(coarse, weights):
    return upsample(coarse) * (weights / upsample(block_mean(weights)))

def smooth(padded, field):
    beside_all = padded[:, :-2, 1:-1] + padded[:, 2:, 1:-1] + padded[:, 1:-1, :-2] + padded[:, 1:-1, 2:]
    return field + diffusion_rate * (beside_all - 4.0 * field)

def route_step(water, moisture, keff, active, codes):
    drained = drainage_rate * active * moisture * moisture
    centre_keff = keff[1:-1, 1:-1]
    centre_water = water[1:-1, 1:-1]
    centre_moist = moisture[1:-1, 1:-1]
    spread = jnp.zeros_like(centre_water)
    for keff_side, water_side in zip(neighbours(keff), neighbours(water)):
        spread = spread + jnp.sqrt(centre_keff * keff_side) * (water_side - centre_water)
    northern, southern, western, eastern = neighbours(drained)
    code_north, code_south, code_west, code_east = neighbours(codes)
    inflow = jnp.where(code_south == 0, southern, 0.0) + jnp.where(code_north == 1, northern, 0.0)
    inflow = inflow + jnp.where(code_east == 2, eastern, 0.0) + jnp.where(code_west == 3, western, 0.0)
    soaked = infiltration_rate * centre_water / (1.0 + centre_moist)
    return (centre_water + spread - soaked, centre_moist + soaked - drained[1:-1, 1:-1] + inflow)

def reference(column_water, land_soil, level_weight, excess_weight, soil_weight, terrain_class, surface_head, conductivity, active_mask, flow_code):
    water = column_water[0]
    for counter in range(SWEEPS):
        water = smooth(jnp.pad(water, ((0, 0), (1, 1), (1, 1))), water)
    precip = lax.optimization_barrier(jnp.sum(level_weight[:, None, None] * water * water, axis=0))
    moisture = land_soil[0]
    excess = precip * moisture * moisture / (moisture * moisture + half_point)
    excess_fine = disaggregate(excess, lookup(excess_weight, terrain_class))
    soil_fine = disaggregate(moisture, lookup(soil_weight, terrain_class))
    active = active_mask[1].astype(jnp.float32)
    keff = conductivity[1] * active
    codes = flow_code[1]
    ponded = active * (surface_head[1] + excess_fine)
    stored = soil_fine
    for counter in range(NSUB):
        ponded, stored = route_step(jnp.pad(ponded, 1), jnp.pad(stored, 1), jnp.pad(keff, 1), jnp.pad(active, 1), jnp.pad(codes, 1))
    land_out = block_mean(stored) / (1.0 + evaporation_scale * water[0] * water[0])
    return jnp.stack([land_out, block_mean(ponded)])
```

```python
import functools

import jax
import jax.numpy as jnp
from jax import lax
from jax.experimental import pallas as pl
from jax.experimental.pallas import tpu as pltpu
from jax.sharding import PartitionSpec as P

AGG = 10
NSUB = 8
SWEEPS = 2

diffusion_rate = 0.2
infiltration_rate = 0.05
drainage_rate = 0.1
half_point = 0.1
evaporation_scale = 0.5

LANE = 128
SUB = 8
MESH = pl.DeviceIdType.MESH
DIRS = ((-1, 0), (1, 0), (0, -1), (0, 1), (-1, -1), (-1, 1), (1, -1), (1, 1))
N, S, W, E, NW, NE, SW, SE = range(8)
OPP = (S, N, E, W, SE, SW, NE, NW)


def iota(shape, dim):
    return lax.broadcasted_iota(jnp.int32, shape, dim)


def pick(table, classes):
    values = [table[k] for k in range(table.shape[0])]
    bit = 1
    while len(values) > 1:
        odd = (classes & bit) != 0
        values = [
            jnp.where(odd, values[k + 1], values[k]) for k in range(0, len(values), 2)
        ]
        bit *= 2
    return values[0]


def halves(x):
    high = x.astype(jnp.bfloat16)
    return high, (x - high.astype(jnp.float32)).astype(jnp.bfloat16)


def kernel(
    ny, nx,
    lw_in, ewt_in, swt_in, water_in, soil_in, terrain_in, head_in, cond_in, active_in, code_in,
    out_ref,
    xi, xf, st, ps, wb, mb, pk, dg, mn, qb, qx, back_tx, back_rx, gather, spreadm,
    lw, ewt, swt, send, recv, local, hop, tab,
):
    group = lax.axis_index("comp")
    gy = lax.axis_index("gy")
    gx = lax.axis_index("gx")
    rows, cols = terrain_in.shape
    lev = water_in.shape[1]
    crow, ccol = soil_in.shape[1], soil_in.shape[2]
    tiles = cols // LANE
    width = tiles + 1
    bands = rows // SUB + 2

    lane = iota((SUB, LANE), 1)
    sub = iota((SUB, LANE), 0)

    def exists(d):
        dy, dx = DIRS[d]
        return (gy + dy >= 0) & (gy + dy < ny) & (gx + dx >= 0) & (gx + dx < nx)

    def at(d):
        dy, dx = DIRS[d]
        return {"comp": group, "gy": gy + dy, "gx": gx + dx}

    partner = {"comp": 1 - group, "gy": gy, "gx": gx}

    def copy(src, dst, d, f):
        return pltpu.make_async_remote_copy(
            src_ref=src, dst_ref=dst, send_sem=send.at[d, f], recv_sem=recv.at[OPP[d], f],
            device_id=at(d), device_id_type=MESH,
        )

    def arrival(dst, d, f):
        return pltpu.make_async_remote_copy(
            src_ref=dst, dst_ref=dst, send_sem=send.at[d, f], recv_sem=recv.at[d, f],
            device_id=at(d), device_id_type=MESH,
        )

    fields = (
        (cond_in.at[0], xf.at[0]),
        (active_in.at[0], xi.at[1]),
        (code_in.at[0], xi.at[2]),
        (head_in.at[0], xf.at[1]),
        (terrain_in, xi.at[0]),
    )
    rfrom = {-1: (0, SUB), 0: (0, rows), 1: (rows - SUB, SUB)}
    cfrom = {-1: (0, LANE), 0: (0, cols), 1: (cols - LANE, LANE)}
    rslot = {-1: (0, SUB), 0: (SUB, rows), 1: (rows + SUB, SUB)}
    cslot = {-1: (cols + LANE, LANE), 0: (0, cols), 1: (cols, LANE)}

    def cut(ref, r, c):
        return ref.at[pl.ds(r[0], r[1]), pl.ds(c[0], c[1])]

    def part(ref, d):
        return cut(ref, rfrom[DIRS[d][0]], cfrom[DIRS[d][1]])

    def slot(ref, d):
        return cut(ref, rslot[DIRS[d][0]], cslot[DIRS[d][1]])

    own = ((SUB, rows), (0, cols))

    def local_copy(src, dst, k):
        return pltpu.make_async_copy(src, dst, local.at[k])

    terrain_load = local_copy(terrain_in, cut(xi.at[0], *own), 4)
    route_loads = [local_copy(f[0], cut(f[1], *own), k) for k, f in enumerate(fields[:4])]
    water_load = local_copy(water_in.at[0], wb.at[8], 0)
    soil_load = local_copy(soil_in.at[0], mb.at[8], 1)

    barrier = pltpu.get_barrier_semaphore()
    for d in range(8):
        @pl.when(exists(d))
        def _():
            pl.semaphore_signal(barrier, inc=1, device_id=at(d), device_id_type=MESH)
    pl.semaphore_signal(barrier, inc=1, device_id=partner, device_id_type=MESH)
    greeted = 1
    for d in range(8):
        greeted = greeted + exists(d).astype(jnp.int32)

    tables = [
        pltpu.make_async_copy(a, b, tab.at[k])
        for k, (a, b) in enumerate(((lw_in, lw), (ewt_in, ewt), (swt_in, swt)))
    ]
    for load in tables:
        load.start()
    terrain_load.start()

    @pl.when(group == 0)
    def _():
        water_load.start()
        soil_load.start()

    @pl.when(group == 1)
    def _():
        for load in route_loads:
            load.start()

    R, AD, M0, M1, M2, M3, EW, HD, SO = range(9)
    WN, WS, WW, WE, AA, B0, B1, B2, B3 = range(9, 18)
    k10 = iota((LANE, ccol), 1) * AGG
    j0 = iota((LANE, ccol), 0)

    for c in range(tiles):
        j = j0 + c * LANE
        gather[c * LANE : (c + 1) * LANE, :] = jnp.where(
            (j >= k10) & (j < k10 + AGG), 1.0, 0.0
        ).astype(jnp.bfloat16)

    @pl.when(group == 1)
    def _():
        kk = iota((2 * ccol, LANE), 0)
        jj = iota((2 * ccol, LANE), 1)
        for c in range(tiles):
            j = jj + c * LANE
            spreadm[:, c * LANE : (c + 1) * LANE] = jnp.where(
                (j >= kk * AGG) & (j < kk * AGG + AGG), 1.0, 0.0
            ).astype(jnp.bfloat16)
        spreadm[:, cols:] = jnp.where(
            ((jj < 64) & (kk == ccol)) | ((jj >= 64) & (kk == 2 * ccol - 1)), 1.0, 0.0
        ).astype(jnp.bfloat16)

        zero = jnp.zeros((SUB, LANE), jnp.float32)
        for c in range(width):
            for edge in (0, (bands + 1) * SUB):
                for k in (R, M0, M1):
                    st[k, c, edge : edge + SUB] = zero
                for k in range(2):
                    for p in range(2):
                        ps[p, k, c, edge : edge + SUB] = zero

    for load in tables:
        load.wait()
    pl.semaphore_wait(barrier, greeted)

    def land_first(d):
        out = [copy(soil_in.at[0], mb.at[OPP[d]], d, 1)]
        if d < 4:
            out.insert(0, copy(water_in.at[0], wb.at[OPP[d]], d, 0))
        return out

    def land_pack(d):
        return copy(pk.at[0 if DIRS[d][1] < 0 else 1], dg.at[OPP[d] - 4], d, 0)

    def land_mean(d):
        return copy(mn.at[8], mn.at[OPP[d]], d, 2)

    def route_sends(d):
        return [copy(part(f[0], d), slot(f[1], OPP[d]), d, k) for k, f in enumerate(fields)]

    q_send = pltpu.make_async_remote_copy(
        src_ref=qb.at[0], dst_ref=qb.at[1], send_sem=hop.at[0], recv_sem=hop.at[1],
        device_id=partner, device_id_type=MESH,
    )
    back_send = pltpu.make_async_remote_copy(
        src_ref=back_tx, dst_ref=back_rx, send_sem=hop.at[2], recv_sem=hop.at[3],
        device_id=partner, device_id_type=MESH,
    )

    def over(dirs, act):
        for d in dirs:
            @pl.when(exists(d))
            def _():
                act(d)

    def start_all(copies):
        for c in copies:
            c.start()

    @pl.when(group == 0)
    def _():
        over(range(8), lambda d: start_all(land_first(d)))

    @pl.when(group == 1)
    def _():
        over(range(8), lambda d: start_all(route_sends(d)))

    def means(first, second):
        parts = []
        for field in (first, second):
            high, low = [], []
            for tile in field:
                a, b = halves(tile)
                high.append(a)
                low.append(b)
            parts.append(jnp.concatenate(high, axis=1))
            parts.append(jnp.concatenate(low, axis=1))
        stacked = jnp.concatenate(parts, axis=0)
        y = jnp.dot(stacked, gather[...], preferred_element_type=jnp.float32)
        i10 = iota((crow, rows), 0) * AGG
        i = iota((crow, rows), 1)
        pool = jnp.where((i >= i10) & (i < i10 + AGG), 1.0, 0.0)
        total = []
        for k in (0, 2):
            z = y[k * rows : (k + 1) * rows] + y[(k + 1) * rows : (k + 2) * rows]
            total.append(
                jnp.dot(pool, z, preferred_element_type=jnp.float32, precision=lax.Precision.HIGHEST)
                * (1.0 / (AGG * AGG))
            )
        return total

    @pl.when(group == 0)
    def _():
        water_load.wait()
        packs = [jnp.zeros((SUB, LANE), jnp.float32), jnp.zeros((SUB, LANE), jnp.float32)]
        for l in range(lev):
            mine = (lane >= 8 * l) & (lane < 8 * l + 8)
            w = wb[8, l]
            packs[0] = jnp.where(mine, pltpu.roll(w, (8 * l) % LANE, 1), packs[0])
            packs[1] = jnp.where(mine, pltpu.roll(w, (8 * l + 8) % LANE, 1), packs[1])
        pk[0] = packs[0]
        pk[1] = packs[1]
        over(range(4, 8), lambda d: land_pack(d).start())

        terrain_load.wait()
        firsts, seconds = [], []
        for c in range(tiles):
            tc = xi[0, SUB : SUB + rows, c * LANE : (c + 1) * LANE]
            firsts.append(pick(ewt, tc))
            seconds.append(pick(swt, tc))
        mean_e, mean_s = means(firsts, seconds)
        mn[8, 0] = mean_e
        mn[8, 1] = mean_s
        over(range(8), lambda d: land_mean(d).start())

        soil_load.wait()
        over(range(4), lambda d: arrival(wb.at[d], d, 0).wait_recv())
        over(range(4, 8), lambda d: arrival(dg.at[d - 4], d, 0).wait_recv())
        over(range(8), lambda d: arrival(mb.at[d], d, 1).wait_recv())

        def valid(a, b):
            r = sub + (0 if a == 0 else jnp.where(sub < 4, crow, -crow))
            r = r + gy * crow
            k = lane + (0 if b == 0 else jnp.where(lane < 64, ccol, -ccol))
            k = k + gx * ccol
            return (r >= 0) & (r < ny * crow) & (k >= 0) & (k < nx * ccol)

        ok = [[valid(a, b) for b in range(2)] for a in range(2)]
        left = lane < 64
        upper = sub < 4

        def joined(get, corner, fill):
            t = [
                [get(8), jnp.where(left, get(E), get(W))],
                [jnp.where(upper, get(S), get(N)), corner],
            ]
            return [[jnp.where(ok[a][b], t[a][b], fill) for b in range(2)] for a in range(2)]

        def corners(get):
            return jnp.where(
                upper,
                jnp.where(left, get(SE), get(SW)),
                jnp.where(left, get(NE), get(NW)),
            )

        def smooth(t):
            new = [[None, None], [None, None]]
            down = [[pltpu.roll(t[a][b], 1, 0) for b in range(2)] for a in range(2)]
            up = [[pltpu.roll(t[a][b], SUB - 1, 0) for b in range(2)] for a in range(2)]
            right = [[pltpu.roll(t[a][b], 1, 1) for b in range(2)] for a in range(2)]
            lft = [[pltpu.roll(t[a][b], LANE - 1, 1) for b in range(2)] for a in range(2)]
            for a in range(2):
                for b in range(2):
                    around = (
                        jnp.where(sub == 0, down[1 - a][b], down[a][b])
                        + jnp.where(sub == SUB - 1, up[1 - a][b], up[a][b])
                        + jnp.where(lane == 0, right[a][1 - b], right[a][b])
                        + jnp.where(lane == LANE - 1, lft[a][1 - b], lft[a][b])
                    )
                    value = t[a][b] + diffusion_rate * (around - 4.0 * t[a][b])
                    new[a][b] = jnp.where(ok[a][b], value, 0.0)
            return new

        ce = jnp.where(upper, dg[SE - 4], dg[NE - 4])
        cw = jnp.where(upper, dg[SW - 4], dg[NW - 4])
        precip = [[0.0, 0.0], [0.0, 0.0]]
        ground = None
        for l in range(lev):
            corner = jnp.where(
                left,
                pltpu.roll(ce, (LANE - 8 * l) % LANE, 1),
                pltpu.roll(cw, (2 * LANE - 8 - 8 * l) % LANE, 1),
            )
            t = joined(lambda k: wb[k, l], corner, 0.0)
            for _ in range(SWEEPS):
                t = smooth(t)
            if l == 0:
                ground = t[0][0]
            for a in range(2):
                for b in range(2):
                    precip[a][b] = precip[a][b] + lw[l] * t[a][b] * t[a][b]

        moisture = joined(lambda k: mb[k], corners(lambda k: mb[k]), 0.5)
        over(range(8), lambda d: arrival(mn.at[d], d, 2).wait_recv())
        m_e = joined(lambda k: mn[k, 0], corners(lambda k: mn[k, 0]), 1.0)
        m_s = joined(lambda k: mn[k, 1], corners(lambda k: mn[k, 1]), 1.0)
        for a in range(2):
            for b in range(2):
                m = moisture[a][b]
                excess = precip[a][b] * m * m / (m * m + half_point)
                rs = slice(a * SUB, (a + 1) * SUB)
                cs = slice(b * LANE, (b + 1) * LANE)
                qb[0, 0, rs, cs] = excess / m_e[a][b]
                qb[0, 1, rs, cs] = m / m_s[a][b]
        q_send.start()
        divisor = 1.0 + evaporation_scale * ground * ground
        over(range(8), lambda d: [c.wait_send() for c in land_first(d)])
        over(range(4, 8), lambda d: land_pack(d).wait_send())
        over(range(8), lambda d: land_mean(d).wait_send())
        q_send.wait_send()
        back_send.wait_recv()
        out_ref[0] = back_rx[...] / divisor


    @pl.when(group == 1)
    def _():
        def prepare(t, c):
            r = pl.ds(t * SUB if isinstance(t, int) else pl.multiple_of(t * SUB, SUB), SUB)
            o = pl.ds(
                (t + 1) * SUB if isinstance(t, int) else pl.multiple_of(t * SUB + SUB, SUB), SUB
            )

            def take(ref, k):
                a = ref[k, r, c * LANE : (c + 1) * LANE]
                if c < tiles:
                    return a
                return jnp.where(lane < 64, a, ref[k, r, (c + 1) * LANE : (c + 2) * LANE])

            row = sub + (t - 1) * SUB + gy * rows
            col = lane + c * LANE
            if c == tiles:
                col = jnp.where(lane < 64, col, lane - LANE)
            col = col + gx * cols
            ok = (row >= 0) & (row < ny * rows) & (col >= 0) & (col < nx * cols)
            active = jnp.where(ok, take(xi, 1).astype(jnp.float32), 0.0)
            code = take(xi, 2)
            keff = jnp.where(ok, take(xf, 0), 0.0) * active
            tc = take(xi, 0)
            st[R, c, o] = jnp.sqrt(keff)
            rate = drainage_rate * active
            st[AD, c, o] = rate
            for k in range(4):
                st[M0 + k, c, o] = jnp.where(code == k, rate, 0.0)
            st[EW, c, o] = active * pick(ewt, tc)
            st[HD, c, o] = active * jnp.where(ok, take(xf, 1), 0.0)
            st[SO, c, o] = pick(swt, tc)

        for load in route_loads:
            load.wait()
        terrain_load.wait()

        def inner(t, carry):
            for c in range(tiles):
                prepare(t, c)
            return carry

        lax.fori_loop(1, bands - 1, inner, 0, unroll=2)

        over(range(8), lambda d: [arrival(slot(f[1], d), d, k).wait_recv() for k, f in enumerate(fields)])

        def rim(k, carry):
            for c in range(tiles):
                prepare(k * (bands - 1), c)
            return carry

        lax.fori_loop(0, 2, rim, 0)

        def side(t, carry):
            prepare(t, tiles)
            return carry

        lax.fori_loop(0, bands, side, 0, unroll=6)

        def from_west(tile_list):
            turned = [pltpu.roll(x, 1, 1) for x in tile_list]
            return [jnp.where(lane == 0, turned[c - 1], turned[c]) for c in range(width)]

        def from_east(tile_list):
            turned = [pltpu.roll(x, LANE - 1, 1) for x in tile_list]
            return [
                jnp.where(lane == LANE - 1, turned[(c + 1) % width], turned[c])
                for c in range(width)
            ]

        def couple(t, carry):
            base = pl.multiple_of(t * SUB + SUB, SUB)
            o = pl.ds(base, SUB)
            above = pl.ds(base - 1, SUB)
            below = pl.ds(base + 1, SUB)
            r = [st[R, c, o] for c in range(width)]
            west, east = from_west(r), from_east(r)
            for c in range(width):
                wn = r[c] * st[R, c, above]
                ws = r[c] * st[R, c, below]
                ww = r[c] * west[c]
                we = r[c] * east[c]
                st[WN, c, o] = wn
                st[WS, c, o] = ws
                st[WW, c, o] = ww
                st[WE, c, o] = we
                st[AA, c, o] = (wn + ws) + (ww + we)
                st[B0, c, o] = st[M0, c, below]
                st[B1, c, o] = st[M1, c, above]
            for c, v in enumerate(from_east([st[M2, c, o] for c in range(width)])):
                st[B2, c, o] = v
            for c, v in enumerate(from_west([st[M3, c, o] for c in range(width)])):
                st[B3, c, o] = v
            return carry

        lax.fori_loop(0, bands, couple, 0, unroll=4)

        q_send.wait_recv()
        high, low = [], []
        for k in range(2):
            a, b = halves(qb[1, k])
            high.append(a)
            low.append(b)
        y = jnp.dot(
            jnp.concatenate(high + low, axis=0), spreadm[...], preferred_element_type=jnp.float32
        )
        qx[...] = y[: 4 * SUB] + y[4 * SUB :]
        for t in range(bands):
            o = slice((t + 1) * SUB, (t + 2) * SUB)
            if t == 0:
                a = b = 2 * crow - 1
            elif t == bands - 1:
                a = b = crow
            else:
                a, b = ((t - 1) * SUB) // AGG, ((t - 1) * SUB + SUB - 1) // AGG
            for c in range(width):
                cs = slice(c * LANE, (c + 1) * LANE)

                def up(k):
                    first = jnp.broadcast_to(qx[k * 16 + a : k * 16 + a + 1, cs], (SUB, LANE))
                    if a == b:
                        return first
                    second = jnp.broadcast_to(qx[k * 16 + b : k * 16 + b + 1, cs], (SUB, LANE))
                    return jnp.where(sub < b * AGG - (t - 1) * SUB, first, second)

                ps[0, 0, c, o] = st[HD, c, o] + st[EW, c, o] * up(0)
                ps[0, 1, c, o] = st[SO, c, o] * up(1)

        def substep(src, dst):
            def band(t, carry):
                base = pl.multiple_of(t * SUB + SUB, SUB)
                o = pl.ds(base, SUB)
                above = pl.ds(base - 1, SUB)
                below = pl.ds(base + 1, SUB)
                p = [ps[src, 0, c, o] for c in range(width)]
                s = [ps[src, 1, c, o] for c in range(width)]
                ss = [x * x for x in s]
                p_w, p_e = from_west(p), from_east(p)
                s_w, s_e = from_west(ss), from_east(ss)
                for c in range(width):
                    s_n = ps[src, 1, c, above]
                    s_s = ps[src, 1, c, below]
                    spread = (
                        st[WN, c, o] * ps[src, 0, c, above]
                        + st[WS, c, o] * ps[src, 0, c, below]
                        + (st[WW, c, o] * p_w[c] + st[WE, c, o] * p_e[c])
                        - st[AA, c, o] * p[c]
                    )
                    soaked = infiltration_rate * p[c] * pl.reciprocal(1.0 + s[c])
                    inflow = (
                        st[B0, c, o] * (s_s * s_s)
                        + st[B1, c, o] * (s_n * s_n)
                        + (st[B2, c, o] * s_e[c] + st[B3, c, o] * s_w[c])
                        - st[AD, c, o] * ss[c]
                    )
                    ps[dst, 0, c, o] = p[c] + (spread - soaked)
                    ps[dst, 1, c, o] = s[c] + (soaked + inflow)
                return carry

            lax.fori_loop(0, bands, band, 0, unroll=12)

        def two(k, carry):
            substep(0, 1)
            substep(1, 0)
            return carry

        lax.fori_loop(0, NSUB // 2, two, 0)

        inside = slice(2 * SUB, 2 * SUB + rows)
        mean_p, mean_st = means(
            [ps[0, 0, c, inside] for c in range(tiles)],
            [ps[0, 1, c, inside] for c in range(tiles)],
        )
        back_tx[...] = mean_st
        back_send.start()
        out_ref[0] = mean_p
        over(range(8), lambda d: [c.wait_send() for c in route_sends(d)])
        back_send.wait_send()


def per_device(ny, nx, column_water, land_soil, level_weight, excess_weight, soil_weight,
               terrain_class, surface_head, conductivity, active_mask, flow_code):
    rows, cols = terrain_class.shape
    lev = column_water.shape[1]
    crow, ccol = land_soil.shape[1:]
    wide = cols // LANE + 1
    tall = rows + 4 * SUB
    f32, i32 = jnp.float32, jnp.int32
    any_spec = pl.BlockSpec(memory_space=pltpu.HBM)
    return pl.pallas_call(
        functools.partial(kernel, ny, nx),
        out_shape=pltpu.VMEM((1, crow, ccol), f32),
        in_specs=[any_spec] * 10,
        out_specs=pl.BlockSpec(memory_space=pltpu.VMEM),
        scratch_shapes=[
            pltpu.VMEM((3, rows + 2 * SUB, cols + 2 * LANE), i32),
            pltpu.VMEM((2, rows + 2 * SUB, cols + 2 * LANE), f32),
            pltpu.VMEM((18, wide, tall, LANE), f32),
            pltpu.VMEM((2, 2, wide, tall, LANE), f32),
            pltpu.VMEM((9, lev, crow, ccol), f32),
            pltpu.VMEM((9, crow, ccol), f32),
            pltpu.VMEM((2, crow, ccol), f32),
            pltpu.VMEM((4, crow, ccol), f32),
            pltpu.VMEM((9, 2, crow, ccol), f32),
            pltpu.VMEM((2, 2, 2 * crow, 2 * ccol), f32),
            pltpu.VMEM((4 * crow, cols + LANE), f32),
            pltpu.VMEM((crow, ccol), f32),
            pltpu.VMEM((crow, ccol), f32),
            pltpu.VMEM((cols, ccol), jnp.bfloat16),
            pltpu.VMEM((2 * ccol, cols + LANE), jnp.bfloat16),
            pltpu.SMEM(level_weight.shape, f32),
            pltpu.SMEM(excess_weight.shape, f32),
            pltpu.SMEM(soil_weight.shape, f32),
            pltpu.SemaphoreType.DMA((8, 5)),
            pltpu.SemaphoreType.DMA((8, 5)),
            pltpu.SemaphoreType.DMA((5,)),
            pltpu.SemaphoreType.DMA((4,)),
            pltpu.SemaphoreType.DMA((3,)),
        ],
        compiler_params=pltpu.CompilerParams(
            collective_id=0, has_side_effects=True
        ),
    )(level_weight, excess_weight, soil_weight, column_water, land_soil, terrain_class,
      surface_head, conductivity, active_mask, flow_code)


def solution(mesh):
    in_specs = (
        P("comp", None, "gy", "gx"),
        P("comp", "gy", "gx"),
        P(),
        P(),
        P(),
        P("gy", "gx"),
        P("comp", "gy", "gx"),
        P("comp", "gy", "gx"),
        P("comp", "gy", "gx"),
        P("comp", "gy", "gx"),
    )
    body = functools.partial(per_device, mesh.shape["gy"], mesh.shape["gx"])
    return jax.shard_map(
        body, mesh=mesh, in_specs=in_specs, out_specs=P("comp", "gy", "gx"), check_vma=False
    )
```

```python
import functools

import jax
import jax.numpy as jnp
from jax import lax
from jax.experimental import pallas as pl
from jax.experimental.pallas import tpu as pltpu
from jax.sharding import PartitionSpec as P

AGG = 10
NSUB = 8
SWEEPS = 2

diffusion_rate = 0.2
infiltration_rate = 0.05
drainage_rate = 0.1
half_point = 0.1
evaporation_scale = 0.5

LANE = 128
SUB = 8
MESH = pl.DeviceIdType.MESH
DIRS = ((-1, 0), (1, 0), (0, -1), (0, 1), (-1, -1), (-1, 1), (1, -1), (1, 1))
N, S, W, E, NW, NE, SW, SE = range(8)
OPP = (S, N, E, W, SE, SW, NE, NW)

R, K, RI, AD, M0, M1, M2, M3, EW, HD, SO, A1 = range(12)
PLANES = 5
U, Y, Q = range(3)
FIELDS = 4


def iota(shape, dim):
    return lax.broadcasted_iota(jnp.int32, shape, dim)


def pick(table, classes):
    values = [table[k] for k in range(table.shape[0])]
    bit = 1
    while len(values) > 1:
        odd = (classes & bit) != 0
        values = [
            jnp.where(odd, values[k + 1], values[k]) for k in range(0, len(values), 2)
        ]
        bit *= 2
    return values[0]


def halves(x):
    high = x.astype(jnp.bfloat16)
    return high, (x - high.astype(jnp.float32)).astype(jnp.bfloat16)


def turn(x, shift):
    shift %= LANE
    return pltpu.roll(x, shift, 1) if shift else x


def kernel(
    ny, nx,
    lw_in, ewt_in, swt_in, water_in, soil_in, terrain_in, head_in, cond_in, active_in, code_in,
    out_ref,
    lw, ewt, swt, xi, act, xf, st, us, wb, mb, wp, wr, pk, pr, fq, fr, qb, back_tx, back_rx,
    gather, perm, planes, hs, hr, sums, sp, sr, cr, send, recv, local, hop,
):
    group = lax.axis_index("comp")
    gy = lax.axis_index("gy")
    gx = lax.axis_index("gx")
    rows, cols = terrain_in.shape
    lev = water_in.shape[1]
    crow, ccol = soil_in.shape[1], soil_in.shape[2]
    tiles = cols // LANE
    width = tiles + 1
    own_bands = rows // SUB
    bands = own_bands + 2

    lane = iota((SUB, LANE), 1)
    sub = iota((SUB, LANE), 0)
    left = lane < LANE // 2
    upper = sub < SUB // 2

    def exists(d):
        dy, dx = DIRS[d]
        return (gy + dy >= 0) & (gy + dy < ny) & (gx + dx >= 0) & (gx + dx < nx)

    def at(d):
        dy, dx = DIRS[d]
        return {"comp": group, "gy": gy + dy, "gx": gx + dx}

    partner = {"comp": 1 - group, "gy": gy, "gx": gx}

    def copy(src, dst, d, f):
        return pltpu.make_async_remote_copy(
            src_ref=src, dst_ref=dst, send_sem=send.at[d, f], recv_sem=recv.at[OPP[d], f],
            device_id=at(d), device_id_type=MESH,
        )

    def arrival(dst, d, f):
        return pltpu.make_async_remote_copy(
            src_ref=dst, dst_ref=dst, send_sem=send.at[d, f], recv_sem=recv.at[d, f],
            device_id=at(d), device_id_type=MESH,
        )

    def across(src, dst, k):
        return pltpu.make_async_remote_copy(
            src_ref=src, dst_ref=dst, send_sem=hop.at[2 * k], recv_sem=hop.at[2 * k + 1],
            device_id=partner, device_id_type=MESH,
        )

    def over(dirs, action):
        for d in dirs:
            @pl.when(exists(d))
            def _():
                action(d)

    def load(src, dst, k):
        return pltpu.make_async_copy(src, dst, local.at[k])

    tables = [load(a, b, k) for k, (a, b) in enumerate(((lw_in, lw), (ewt_in, ewt), (swt_in, swt)))]
    terrain_load = load(terrain_in, xi.at[0], 3)
    land_loads = [load(water_in.at[0], wb, 4), load(soil_in.at[0], mb, 5)]
    route_loads = [
        load(cond_in.at[0], xf.at[0], 4),
        load(active_in.at[0], act, 5),
        load(code_in.at[0], xi.at[1], 6),
        load(head_in.at[0], xf.at[1], 7),
    ]

    barrier = pltpu.get_barrier_semaphore()
    greeted = 1
    for d in range(8):
        meet = exists(d) if d < 4 else exists(d) & (group == 0)
        greeted = greeted + meet.astype(jnp.int32)

        @pl.when(meet)
        def _():
            pl.semaphore_signal(barrier, inc=1, device_id=at(d), device_id_type=MESH)
    pl.semaphore_signal(barrier, inc=1, device_id=partner, device_id_type=MESH)

    for c in tables:
        c.start()

    @pl.when(group == 0)
    def _():
        terrain_load.start()
        for c in land_loads:
            c.start()

    @pl.when(group == 1)
    def _():
        for c in route_loads:
            c.start()
        terrain_load.start()

    def land_sends(d):
        if d < 2:
            return [copy(wp.at[d], wr.at[OPP[d]], d, 0), copy(fq, fr.at[OPP[d]], d, 1)]
        return [copy(pk.at[0 if DIRS[d][1] < 0 else 1], pr.at[OPP[d]], d, 0)]

    def land_arrivals(d):
        if d < 2:
            return [arrival(wr.at[d], d, 0), arrival(fr.at[d], d, 1)]
        return [arrival(pr.at[d], d, 0)]

    def route_sends(d):
        if d < 2:
            return [copy(hs.at[d], hr.at[OPP[d]], d, 0)]
        return [copy(sp.at[d - 2], sr.at[OPP[d] - 2], d, 0)]

    def route_arrivals(d):
        return [arrival(hr.at[d] if d < 2 else sr.at[d - 2], d, 0)]

    def corner_send(d, s):
        return copy(sr.at[s, 0], cr.at[OPP[d], s], d, 1 + s)

    def corner_arrival(d, s):
        return arrival(cr.at[d, s], d, 1 + s)

    def corners(action):
        for d in (N, S):
            for s in (0, 1):
                @pl.when(exists(d) & exists(W + s))
                def _():
                    action(d, s)

    s_send = across(qb.at[1, 0], qb.at[1, 1], 0)
    e_send = across(qb.at[0, 0], qb.at[0, 1], 1)
    back_send = across(back_tx, back_rx, 2)

    def mean(field):
        parts = [halves(tile) for tile in field]
        stacked = jnp.concatenate(
            [jnp.concatenate([p[k] for p in parts], axis=1) for k in (0, 1)], axis=0
        )
        y = jnp.dot(stacked, gather[...], preferred_element_type=jnp.float32)
        return pool(y[:rows] + y[rows:], 1.0)

    def pool(z, scale):
        i10 = iota((crow, rows), 0) * AGG
        i = iota((crow, rows), 1)
        ones = jnp.where((i >= i10) & (i < i10 + AGG), 1.0, 0.0).astype(jnp.bfloat16)
        high, low = halves(z)
        return jnp.dot(
            jnp.concatenate([ones, ones], axis=1), jnp.concatenate([high, low], axis=0),
            preferred_element_type=jnp.float32,
        ) * (scale / (AGG * AGG))

    def unpack(east, west, g):
        return jnp.where(left, turn(east, -SUB * g), turn(west, -SUB * g - SUB))

    @pl.when(group == 0)
    def _():
        k10 = iota((LANE, ccol), 1) * AGG
        j0 = iota((LANE, ccol), 0)
        for c in range(tiles):
            j = j0 + c * LANE
            gather[c * LANE : (c + 1) * LANE, :] = jnp.where(
                (j >= k10) & (j < k10 + AGG), 1.0, 0.0
            ).astype(jnp.bfloat16)
        for c in land_loads:
            c.wait()
        packs = [jnp.zeros((SUB, LANE), jnp.float32)] * 2
        for l in range(lev):
            mine = (lane >= SUB * l) & (lane < SUB * l + SUB)
            w = wb[l]
            packs[0] = jnp.where(mine, turn(w, SUB * l), packs[0])
            packs[1] = jnp.where(mine, turn(w, SUB * l + SUB), packs[1])
        pk[0, 0] = packs[0]
        pk[1, 0] = packs[1]
        for i in range(lev // 2):
            a, b = wb[2 * i], wb[2 * i + 1]
            wp[N, i] = jnp.where(upper, a, pltpu.roll(b, SUB // 2, 0))
            wp[S, i] = jnp.where(upper, pltpu.roll(a, SUB // 2, 0), b)

        for c in tables:
            c.wait()
        terrain_load.wait()
        firsts, seconds = [], []
        for c in range(tiles):
            tc = xi[0, :, c * LANE : (c + 1) * LANE]
            firsts.append(pick(ewt, tc))
            seconds.append(pick(swt, tc))
        m = mb[...]
        mm = m * m
        own_f = mm / ((mm + half_point) * mean(firsts))
        own_q = m / mean(seconds)
        fq[0] = own_f
        fq[1] = own_q
        for side in range(2):
            a, b = turn(own_f, SUB * side), turn(own_q, SUB * side + SUB)
            pk[side, 1] = jnp.where(lane < SUB, a, b)

        pl.semaphore_wait(barrier, greeted)
        over((4, 5, 6, 7, 2, 3, 0, 1), lambda d: [c.start() for c in land_sends(d)])

        def valid(a, b):
            r = sub + (0 if a == 0 else jnp.where(upper, crow, -crow)) + gy * crow
            k = lane + (0 if b == 0 else jnp.where(left, ccol, -ccol)) + gx * ccol
            return (r >= 0) & (r < ny * crow) & (k >= 0) & (k < nx * ccol)

        ok = [[valid(a, b) for b in range(2)] for a in range(2)]
        over(range(8), lambda d: [c.wait_recv() for c in land_arrivals(d)])

        def joined(own, ns, k, g):
            ce = jnp.where(upper, pr[SE, k], pr[NE, k])
            cw = jnp.where(upper, pr[SW, k], pr[NW, k])
            t = [[own, unpack(pr[E, k], pr[W, k], g)], [ns, unpack(ce, cw, g)]]
            return [[jnp.where(ok[a][b], t[a][b], 0.0) for b in range(2)] for a in range(2)]

        ratio = [
            joined(fq[f], jnp.where(upper, fr[S, f], fr[N, f]), 1, f) for f in range(2)
        ]
        def hand(k, t):
            for a in range(2):
                edge = jnp.where(
                    left, jnp.broadcast_to(t[a][1][:, :1], (SUB, LANE)),
                    jnp.broadcast_to(t[a][1][:, LANE - 1 :], (SUB, LANE)),
                )
                for b, v in enumerate((t[a][0], edge)):
                    qb[k, 0, a * SUB : (a + 1) * SUB, b * LANE : (b + 1) * LANE] = v

        hand(1, ratio[1])
        s_send.start()

        def smooth(t):
            new = [[None, None], [None, None]]
            down = [[pltpu.roll(t[a][b], 1, 0) for b in range(2)] for a in range(2)]
            up = [[pltpu.roll(t[a][b], SUB - 1, 0) for b in range(2)] for a in range(2)]
            right = [[pltpu.roll(t[a][b], 1, 1) for b in range(2)] for a in range(2)]
            lft = [[pltpu.roll(t[a][b], LANE - 1, 1) for b in range(2)] for a in range(2)]
            for a in range(2):
                for b in range(2):
                    around = (
                        jnp.where(sub == 0, down[1 - a][b], down[a][b])
                        + jnp.where(sub == SUB - 1, up[1 - a][b], up[a][b])
                        + jnp.where(lane == 0, right[a][1 - b], right[a][b])
                        + jnp.where(lane == LANE - 1, lft[a][1 - b], lft[a][b])
                    )
                    value = t[a][b] + diffusion_rate * (around - 4.0 * t[a][b])
                    new[a][b] = jnp.where(ok[a][b], value, 0.0)
            return new

        precip = [[0.0, 0.0], [0.0, 0.0]]
        ground = None
        for l in range(lev):
            n, s = wr[N, l // 2], wr[S, l // 2]
            if l % 2 == 0:
                n = pltpu.roll(n, SUB // 2, 0)
            else:
                s = pltpu.roll(s, SUB // 2, 0)
            t = joined(wb[l], jnp.where(upper, s, n), 0, l)
            for _ in range(SWEEPS):
                t = smooth(t)
            if l == 0:
                ground = t[0][0]
            for a in range(2):
                for b in range(2):
                    precip[a][b] = precip[a][b] + lw[l] * t[a][b] * t[a][b]

        hand(0, [[precip[a][b] * ratio[0][a][b] for b in range(2)] for a in range(2)])
        e_send.start()
        divisor = 1.0 + evaporation_scale * ground * ground
        over(range(8), lambda d: [c.wait_send() for c in land_sends(d)])
        s_send.wait_send()
        e_send.wait_send()
        back_send.wait_recv()
        out_ref[0] = back_rx[...] / divisor

    @pl.when(group == 1)
    def _():
        at_c = iota((2 * SUB, LANE), 1) * AGG - iota((2 * SUB, LANE), 0)

        def place(k, carry):
            j = pl.multiple_of(k * 2 * SUB, 2 * SUB)
            for c in range(tiles):
                perm[pl.ds(j, 2 * SUB), c * LANE : (c + 1) * LANE] = jnp.where(
                    at_c == j - c, 1.0, 0.0
                ).astype(jnp.bfloat16)
            return carry

        lax.fori_loop(0, cols // (2 * SUB), place, 0, unroll=4)
        zero = jnp.zeros((SUB, LANE), jnp.float32)
        for c in range(width):
            for edge in (0, (bands + 1) * SUB):
                for k in (R, M0, M1):
                    st[k, c, edge : edge + SUB] = zero
                for k in (U, Q):
                    for p in range(2):
                        us[p, k, c, edge : edge + SUB] = zero

        for c in route_loads:
            c.wait()
        terrain_load.wait()

        def stage(keff, code, head, tc):
            mixed = (code + 4 * tc).astype(jnp.float32).astype(jnp.bfloat16)
            return [mixed, *halves(keff), *halves(head)]

        def unmix(v, m, k, cs):
            got = [v[p * m + k : p * m + k + SUB, cs] for p in range(PLANES)]
            mixed = got[0].astype(jnp.int32)
            return got[1] + got[2], mixed & 3, got[3] + got[4], mixed >> 2

        chunk = 2 * LANE
        ends = (0, rows - SUB)

        def both(ref, *lead):
            return jnp.concatenate([ref[(*lead, slice(e, e + SUB))] for e in ends], axis=0)

        edge = jnp.concatenate(
            stage(both(xf, 0) * both(act).astype(jnp.float32), both(xi, 1), both(xf, 1), both(xi, 0)),
            axis=0,
        )
        for n in range(0, cols, chunk):
            v = jnp.dot(edge, perm[:, n : n + chunk], preferred_element_type=jnp.float32)
            for c in range(n // LANE, (n + chunk) // LANE):
                cs = slice(c * LANE - n, c * LANE - n + LANE)
                for d in (N, S):
                    for f, x in enumerate(unmix(v, 2 * SUB, d * SUB, cs)):
                        hs[d, f, c] = x.astype(jnp.float32)

        order = [0, own_bands - 1] + list(range(1, own_bands - 1))
        for side in range(2):
            cs = slice(0, LANE) if side == 0 else slice(cols - LANE, cols)
            for q in range(sp.shape[1]):
                tile = zero
                for i, b in enumerate(order[4 * q : 4 * q + 4]):
                    o = slice(b * SUB, b * SUB + SUB)
                    keff = xf[0, o, cs] * act[o, cs].astype(jnp.float32)
                    values = (
                        keff, xi[1, o, cs].astype(jnp.float32), xf[1, o, cs],
                        xi[0, o, cs].astype(jnp.float32),
                    )
                    for f, v in enumerate(values):
                        g = i * FIELDS + f
                        tile = jnp.where(
                            (lane >= SUB * g) & (lane < SUB * g + SUB),
                            turn(v, SUB * g + SUB * side), tile,
                        )
                sp[side, q] = tile

        pl.semaphore_wait(barrier, greeted)
        over((2, 3, 0, 1), lambda d: [c.start() for c in route_sends(d)])
        for c in tables:
            c.wait()

        def put(c, o, keff, head, code, tc):
            live = keff > 0.0
            rs = lax.rsqrt(jnp.where(live, keff, 1.0))
            r = keff * rs
            rate = jnp.where(live, drainage_rate * infiltration_rate, 0.0)
            st[R, c, o] = r
            st[K, c, o] = keff
            st[RI, c, o] = jnp.where(live, rs * (1.0 / infiltration_rate), 0.0)
            st[AD, c, o] = rate
            for k in range(4):
                st[M0 + k, c, o] = jnp.where(code == k, rate, 0.0)
            st[EW, c, o] = r * pick(ewt, tc)
            st[HD, c, o] = r * head
            st[SO, c, o] = pick(swt, tc) * (1.0 / infiltration_rate)

        def aligned(x):
            return x if isinstance(x, int) else pl.multiple_of(x, SUB)

        middle = rows - 2 * SUB
        for i in range(0, middle, 2 * SUB):
            o = slice(SUB + i, 3 * SUB + i)
            parts = stage(xf[0, o] * act[o].astype(jnp.float32), xi[1, o], xf[1, o], xi[0, o])
            for p, x in enumerate(parts):
                planes[p * middle + i : p * middle + i + 2 * SUB, :] = x
        for n in range(0, cols, chunk):
            v = jnp.dot(planes[...], perm[:, n : n + chunk], preferred_element_type=jnp.float32)
            for c in range(n // LANE, (n + chunk) // LANE):
                cs = slice(c * LANE - n, c * LANE - n + LANE)
                for t in range(2, bands - 2):
                    keff, code, head, tc = unmix(v, middle, (t - 2) * SUB, cs)
                    put(c, slice(t * SUB + SUB, t * SUB + 2 * SUB), keff, head, code, tc)

        def put_row(t, ref, d, there):
            for c in range(tiles):
                keff, code, head, tc = [
                    jnp.where((lane >= 0) & there, ref[d, f, c], 0.0) for f in range(FIELDS)
                ]
                put(c, slice(t * SUB + SUB, t * SUB + 2 * SUB), keff, head, code,
                    tc.astype(jnp.int32))

        yes = gy >= 0
        put_row(1, hs, N, yes)
        put_row(bands - 2, hs, S, yes)

        over((W, E), lambda d: [c.wait_recv() for c in route_arrivals(d)])
        corners(lambda d, s: corner_send(d, s).start())

        def side_ok(there):
            reach = (lane < SUB) & exists(E) | (lane >= LANE - SUB) & exists(W)
            return reach & there

        def put_side(t, east, west, g, there):
            ok = side_ok(there)
            keff, code, head, tc = [unpack(east, west, g + f) for f in range(FIELDS)]
            put(
                tiles, slice(t * SUB + SUB, t * SUB + 2 * SUB), jnp.where(ok, keff, 0.0),
                jnp.where(ok, head, 0.0), jnp.where(ok, code, 0.0),
                jnp.where(ok, tc, 0.0).astype(jnp.int32),
            )

        for i, b in enumerate(order):
            put_side(b + 1, sr[1, i // 4], sr[0, i // 4], (i % 4) * FIELDS, yes)

        def beside(west_of, east_of):
            w, e = west_of, east_of
            last = tiles - 1
            w_end, w_side = pltpu.roll(w[last], 1, 1), pltpu.roll(w[tiles], 1, 1)
            e_end, e_side = pltpu.roll(e[0], LANE - 1, 1), pltpu.roll(e[tiles], LANE - 1, 1)
            first, final = lane == 0, lane == LANE - 1
            west = [jnp.where(first, w_side, w_end), *w[:last], jnp.where(first, w_end, w_side)]
            east = [*e[1:tiles], jnp.where(final, e_side, e_end), jnp.where(final, e_end, e_side)]
            return west, east

        def around(t):
            base = aligned(t * SUB + SUB)
            return pl.ds(base, SUB), pl.ds(base - 1, SUB), pl.ds(base + 1, SUB)

        def couple(t, carry):
            o, above, below = around(t)
            r = [st[R, c, o] for c in range(width)]
            west, east = beside(r, r)
            for c in range(width):
                total = (st[R, c, above] + st[R, c, below]) + (west[c] + east[c])
                st[A1, c, o] = 1.0 - r[c] * total
            return carry

        lax.fori_loop(2, bands - 2, couple, 0, unroll=2)

        over((N, S), lambda d: [c.wait_recv() for c in route_arrivals(d)])
        corners(lambda d, s: corner_arrival(d, s).wait_recv())
        for t, d, g in ((0, N, FIELDS), (bands - 1, S, 0)):
            put_row(t, hr, d, exists(d))
            put_side(t, cr[d, 1], cr[d, 0], g, exists(d))
        for t in (0, 1, bands - 2, bands - 1):
            couple(t, 0)

        def up(k, t):
            if t == 0:
                a = b = 2 * crow - 1
            elif t == bands - 1:
                a = b = crow
            else:
                a, b = ((t - 1) * SUB) // AGG, ((t - 1) * SUB + SUB - 1) // AGG
            got = []
            for side in range(2):
                cs = slice(side * LANE, side * LANE + LANE)
                v = jnp.broadcast_to(qb[k, 1, a : a + 1, cs], (SUB, LANE))
                if a != b:
                    second = jnp.broadcast_to(qb[k, 1, b : b + 1, cs], (SUB, LANE))
                    v = jnp.where(sub < b * AGG - (t - 1) * SUB, v, second)
                got.append(v)
            return [got[0]] * tiles + [got[1]]

        s_send.wait_recv()
        for t in range(bands):
            o = slice((t + 1) * SUB, (t + 2) * SUB)
            for c, v in enumerate(up(1, t)):
                y = st[SO, c, o] * v
                us[0, Y, c, o] = y
                us[0, Q, c, o] = y * y

        e_send.wait_recv()
        for t in range(bands):
            o = slice((t + 1) * SUB, (t + 2) * SUB)
            for c, v in enumerate(up(0, t)):
                us[0, U, c, o] = st[HD, c, o] + st[EW, c, o] * v

        full = 1.0 / infiltration_rate

        def flows(src, o):
            q = [us[src, Q, c, o] for c in range(width)]
            return beside(
                [st[M3, c, o] * q[c] for c in range(width)],
                [st[M2, c, o] * q[c] for c in range(width)],
            )

        def soak(src, c, o):
            return us[src, U, c, o] * pl.reciprocal(us[src, Y, c, o] + full)

        def new_y(src, c, o, above, below, gu, sides):
            return (
                (us[src, Y, c, o] + st[RI, c, o] * gu)
                + (st[M0, c, below] * us[src, Q, c, below] + st[M1, c, above] * us[src, Q, c, above])
                + ((sides[0][c] + sides[1][c]) - st[AD, c, o] * us[src, Q, c, o])
            )

        def new_u(src, c, o, above, below, gu, sides):
            total = (us[src, U, c, above] + us[src, U, c, below]) + (sides[0][c] + sides[1][c])
            return (st[A1, c, o] * us[src, U, c, o] - gu) + st[K, c, o] * total

        def sides_u(src, o):
            u = [us[src, U, c, o] for c in range(width)]
            return beside(u, u)

        def substep(src, dst):
            def band(t, carry):
                o, above, below = around(t)
                u_sides, q_sides = sides_u(src, o), flows(src, o)
                for c in range(width):
                    gu = soak(src, c, o)
                    y = new_y(src, c, o, above, below, gu, q_sides)
                    us[dst, U, c, o] = new_u(src, c, o, above, below, gu, u_sides)
                    us[dst, Y, c, o] = y
                    us[dst, Q, c, o] = y * y
                return carry

            lax.fori_loop(0, bands, band, 0, unroll=UNROLL)

        def two(k, carry):
            substep(0, 1)
            substep(1, 0)
            return carry

        lax.fori_loop(0, NSUB // 2 - 1, two, 0)
        substep(0, 1)

        def last_y(t, carry):
            o, above, below = around(t)
            q_sides = flows(1, o)
            total = None
            for c in range(tiles):
                y = new_y(1, c, o, above, below, soak(1, c, o), q_sides)
                total = y if total is None else total + y
            sums[0, pl.ds(aligned(t * SUB - SUB), SUB)] = total
            return carry

        def last_u(t, carry):
            o, above, below = around(t)
            u_sides = sides_u(1, o)
            total = None
            for c in range(tiles):
                p = new_u(1, c, o, above, below, soak(1, c, o), u_sides) * st[RI, c, o]
                total = p if total is None else total + p
            sums[1, pl.ds(aligned(t * SUB - SUB), SUB)] = total
            return carry

        lax.fori_loop(1, bands - 1, last_y, 0, unroll=True)
        back_tx[...] = pool(sums[0], infiltration_rate)
        back_send.start()
        lax.fori_loop(1, bands - 1, last_u, 0, unroll=True)
        out_ref[0] = pool(sums[1], infiltration_rate)
        over(range(4), lambda d: [c.wait_send() for c in route_sends(d)])
        corners(lambda d, s: corner_send(d, s).wait_send())
        back_send.wait_send()


UNROLL = 4


def per_device(ny, nx, column_water, land_soil, level_weight, excess_weight, soil_weight,
               terrain_class, surface_head, conductivity, active_mask, flow_code):
    rows, cols = terrain_class.shape
    lev = column_water.shape[1]
    crow, ccol = land_soil.shape[1:]
    wide = cols // LANE + 1
    tall = rows + 4 * SUB
    packs = -(-(rows // SUB) // 4)
    f32, i32, bf16 = jnp.float32, jnp.int32, jnp.bfloat16
    hbm = pl.BlockSpec(memory_space=pltpu.HBM)
    return pl.pallas_call(
        functools.partial(kernel, ny, nx),
        out_shape=pltpu.VMEM((1, crow, ccol), f32),
        in_specs=[hbm] * 10,
        out_specs=pl.BlockSpec(memory_space=pltpu.VMEM),
        scratch_shapes=[
            pltpu.SMEM(level_weight.shape, f32),
            pltpu.SMEM(excess_weight.shape, f32),
            pltpu.SMEM(soil_weight.shape, f32),
            pltpu.VMEM((2, rows, cols), i32),
            pltpu.VMEM((rows, cols), i32),
            pltpu.VMEM((2, rows, cols), f32),
            pltpu.VMEM((12, wide, tall, LANE), f32),
            pltpu.VMEM((2, 3, wide, tall, LANE), f32),
            pltpu.VMEM((lev, crow, ccol), f32),
            pltpu.VMEM((crow, ccol), f32),
            pltpu.VMEM((2, lev // 2, crow, ccol), f32),
            pltpu.VMEM((2, lev // 2, crow, ccol), f32),
            pltpu.VMEM((2, 2, crow, ccol), f32),
            pltpu.VMEM((8, 2, crow, ccol), f32),
            pltpu.VMEM((2, crow, ccol), f32),
            pltpu.VMEM((2, 2, crow, ccol), f32),
            pltpu.VMEM((2, 2, 2 * crow, 2 * ccol), f32),
            pltpu.VMEM((crow, ccol), f32),
            pltpu.VMEM((crow, ccol), f32),
            pltpu.VMEM((cols, ccol), bf16),
            pltpu.VMEM((cols, cols), bf16),
            pltpu.VMEM((PLANES * (rows - 2 * SUB), cols), bf16),
            pltpu.VMEM((2, FIELDS, wide - 1, SUB, LANE), f32),
            pltpu.VMEM((2, FIELDS, wide - 1, SUB, LANE), f32),
            pltpu.VMEM((2, rows, LANE), f32),
            pltpu.VMEM((2, packs, SUB, LANE), f32),
            pltpu.VMEM((2, packs, SUB, LANE), f32),
            pltpu.VMEM((2, 2, SUB, LANE), f32),
            pltpu.SemaphoreType.DMA((8, 3)),
            pltpu.SemaphoreType.DMA((8, 3)),
            pltpu.SemaphoreType.DMA((8,)),
            pltpu.SemaphoreType.DMA((6,)),
        ],
        compiler_params=pltpu.CompilerParams(
            collective_id=0, has_side_effects=True
        ),
    )(level_weight, excess_weight, soil_weight, column_water, land_soil, terrain_class,
      surface_head, conductivity, active_mask, flow_code)


def solution(mesh):
    in_specs = (
        P("comp", None, "gy", "gx"),
        P("comp", "gy", "gx"),
        P(),
        P(),
        P(),
        P("gy", "gx"),
        P("comp", "gy", "gx"),
        P("comp", "gy", "gx"),
        P("comp", "gy", "gx"),
        P("comp", "gy", "gx"),
    )
    body = functools.partial(per_device, mesh.shape["gy"], mesh.shape["gx"])
    return jax.shard_map(
        body, mesh=mesh, in_specs=in_specs, out_specs=P("comp", "gy", "gx"), check_vma=False
    )
```

```python
import functools

import jax
import jax.numpy as jnp
from jax import lax
from jax.experimental import pallas as pl
from jax.experimental.pallas import tpu as pltpu
from jax.sharding import PartitionSpec as P

AGG = 10
NSUB = 8
SWEEPS = 2

diffusion_rate = 0.2
infiltration_rate = 0.05
drainage_rate = 0.1
half_point = 0.1
evaporation_scale = 0.5

LANE = 128
SUB = 8
MESH = pl.DeviceIdType.MESH
DIRS = ((-1, 0), (1, 0), (0, -1), (0, 1), (-1, -1), (-1, 1), (1, -1), (1, 1))
N, S, W, E, NW, NE, SW, SE = range(8)
OPP = (S, N, E, W, SE, SW, NE, NW)

R, K, RI, AD, M0, M1, M2, EW, HD, SO, A1 = range(11)
PLANES = 5
U, Y, Q = range(3)
FIELDS = 4


def iota(shape, dim):
    return lax.broadcasted_iota(jnp.int32, shape, dim)


def pick(lanes, classes):
    return jnp.take_along_axis(lanes, classes, axis=1, mode="promise_in_bounds")


def halves(x):
    high = x.astype(jnp.bfloat16)
    return high, (x - high.astype(jnp.float32)).astype(jnp.bfloat16)


def turn(x, shift):
    shift %= LANE
    return pltpu.roll(x, shift, 1) if shift else x


def kernel(
    ny, nx,
    lw_in, ewt_in, swt_in, water_in, soil_in, terrain_in, head_in, cond_in, active_in, code_in,
    out_ref,
    lw, ewt, swt, xi, act, xf, st, us, wb, mb, wp, wr, pk, pr, fq, fr, qb, back_tx, back_rx,
    gather, perm, planes, hs, hr, sums, sp, sr, cr, send, recv, local, hop,
):
    group = lax.axis_index("comp")
    gy = lax.axis_index("gy")
    gx = lax.axis_index("gx")
    rows, cols = terrain_in.shape
    lev = water_in.shape[1]
    crow, ccol = soil_in.shape[1], soil_in.shape[2]
    tiles = cols // LANE
    width = tiles + 1
    own_bands = rows // SUB
    bands = own_bands + 2

    lane = iota((SUB, LANE), 1)
    sub = iota((SUB, LANE), 0)
    left = lane < LANE // 2
    upper = sub < SUB // 2

    def exists(d):
        dy, dx = DIRS[d]
        return (gy + dy >= 0) & (gy + dy < ny) & (gx + dx >= 0) & (gx + dx < nx)

    def at(d):
        dy, dx = DIRS[d]
        return {"comp": group, "gy": gy + dy, "gx": gx + dx}

    partner = {"comp": 1 - group, "gy": gy, "gx": gx}

    def copy(src, dst, d, f):
        return pltpu.make_async_remote_copy(
            src_ref=src, dst_ref=dst, send_sem=send.at[d, f], recv_sem=recv.at[OPP[d], f],
            device_id=at(d), device_id_type=MESH,
        )

    def arrival(dst, d, f):
        return pltpu.make_async_remote_copy(
            src_ref=dst, dst_ref=dst, send_sem=send.at[d, f], recv_sem=recv.at[d, f],
            device_id=at(d), device_id_type=MESH,
        )

    def across(src, dst, k):
        return pltpu.make_async_remote_copy(
            src_ref=src, dst_ref=dst, send_sem=hop.at[2 * k], recv_sem=hop.at[2 * k + 1],
            device_id=partner, device_id_type=MESH,
        )

    def spread_table(table):
        v = jnp.zeros((SUB, LANE), jnp.float32)
        for k in range(table.shape[0]):
            v = jnp.where(lane == k, table[k], v)
        return v

    def over(dirs, action):
        for d in dirs:
            @pl.when(exists(d))
            def _():
                action(d)

    def load(src, dst, k):
        return pltpu.make_async_copy(src, dst, local.at[k])

    tables = [load(a, b, k) for k, (a, b) in enumerate(((lw_in, lw), (ewt_in, ewt), (swt_in, swt)))]
    terrain_load = load(terrain_in, xi.at[0], 3)
    land_loads = [load(water_in.at[0], wb, 4), load(soil_in.at[0], mb, 5)]
    ends = (0, rows - SUB)
    bulk = [
        (cond_in.at[0], xf.at[0]), (active_in.at[0], act), (code_in.at[0], xi.at[1]),
        (head_in.at[0], xf.at[1]), (terrain_in, xi.at[0]),
    ]

    def some(refs, start, size, k):
        return load(*[r.at[pl.ds(start, size)] for r in refs], k)

    edges = [some(r, e, SUB, 3 + 2 * k + i) for k, r in enumerate(bulk) for i, e in enumerate(ends)]
    rest = [some(r, SUB, rows - 2 * SUB, 13 + k) for k, r in enumerate(bulk)]

    barrier = pltpu.get_barrier_semaphore()
    greeted = 1
    for d in range(8):
        meet = exists(d) if d < 4 else exists(d) & (group == 0)
        greeted = greeted + meet.astype(jnp.int32)

        @pl.when(meet)
        def _():
            pl.semaphore_signal(barrier, inc=1, device_id=at(d), device_id_type=MESH)
    pl.semaphore_signal(barrier, inc=1, device_id=partner, device_id_type=MESH)

    @pl.when(group == 0)
    def _():
        for c in land_loads:
            c.start()
        terrain_load.start()

    @pl.when(group == 1)
    def _():
        for c in edges + rest:
            c.start()

    for c in tables:
        c.start()

    def land_sends(d):
        if d < 2:
            return [copy(wp.at[d], wr.at[OPP[d]], d, 0), copy(fq, fr.at[OPP[d]], d, 1)]
        side = 0 if DIRS[d][1] < 0 else 1
        return [copy(pk.at[side, k], pr.at[OPP[d], k], d, k) for k in range(2)]

    def land_arrivals(d):
        if d < 2:
            return [arrival(wr.at[d], d, 0), arrival(fr.at[d], d, 1)]
        return [arrival(pr.at[d, k], d, k) for k in range(2)]

    def route_sends(d):
        if d < 2:
            return [copy(hs.at[d], hr.at[OPP[d]], d, 0)]
        return [copy(sp.at[d - 2], sr.at[OPP[d] - 2], d, 0)]

    def route_arrivals(d):
        return [arrival(hr.at[d] if d < 2 else sr.at[d - 2], d, 0)]

    def corner_send(d, s):
        return copy(sr.at[s, 0], cr.at[OPP[d], s], d, 1 + s)

    def corner_arrival(d, s):
        return arrival(cr.at[d, s], d, 1 + s)

    def corners(action):
        for d in (N, S):
            for s in (0, 1):
                @pl.when(exists(d) & exists(W + s))
                def _():
                    action(d, s)

    s_send = across(qb.at[1, 0, pl.ds(0, SUB)], qb.at[1, 1, pl.ds(0, SUB)], 0)
    e_send = across(qb.at[0, 0], qb.at[0, 1], 1)
    back_send = across(back_tx, back_rx, 2)

    def pool_rows():
        i10 = iota((crow, rows), 0) * AGG
        i = iota((crow, rows), 1)
        ones = jnp.where((i >= i10) & (i < i10 + AGG), 1.0, 0.0).astype(jnp.bfloat16)
        return jnp.concatenate([ones, ones], axis=1)

    def pool(z, scale):
        return jnp.dot(
            pool_rows(), jnp.concatenate(halves(z), axis=0), preferred_element_type=jnp.float32
        ) * (scale / (AGG * AGG))

    def block_means(fields):
        ones = pool_rows()
        summed = []
        for field in fields:
            parts = [jnp.concatenate(halves(tile), axis=0) for tile in field]
            summed.append(
                jnp.dot(ones, jnp.concatenate(parts, axis=1), preferred_element_type=jnp.float32)
            )
        stacked = jnp.concatenate(halves(jnp.concatenate(summed, axis=0)), axis=0)
        y = jnp.dot(stacked, gather[...], preferred_element_type=jnp.float32)
        total = (y[: 2 * crow] + y[2 * crow :]) * (1.0 / (AGG * AGG))
        return total[:crow], total[crow:]

    def unpack(east, west, g):
        return jnp.where(left, turn(east, -SUB * g), turn(west, -SUB * g - SUB))

    @pl.when(group == 0)
    def _():
        for c in land_loads:
            c.wait()
        packs = [jnp.zeros((SUB, LANE), jnp.float32)] * 2
        for l in range(lev):
            mine = (lane >= SUB * l) & (lane < SUB * l + SUB)
            w = wb[l]
            packs[0] = jnp.where(mine, turn(w, SUB * l), packs[0])
            packs[1] = jnp.where(mine, turn(w, SUB * l + SUB), packs[1])
        pk[0, 0] = packs[0]
        pk[1, 0] = packs[1]
        for i in range(lev // 2):
            a, b = wb[2 * i], wb[2 * i + 1]
            wp[N, i] = jnp.where(upper, a, pltpu.roll(b, SUB // 2, 0))
            wp[S, i] = jnp.where(upper, pltpu.roll(a, SUB // 2, 0), b)

        pl.semaphore_wait(barrier, greeted)
        over((0, 1, 4, 5, 6, 7, 2, 3), lambda d: land_sends(d)[0].start())

        k10 = iota((LANE, ccol), 1) * AGG
        j0 = iota((LANE, ccol), 0)
        for c in range(tiles):
            j = j0 + c * LANE
            gather[c * LANE : (c + 1) * LANE, :] = jnp.where(
                (j >= k10) & (j < k10 + AGG), 1.0, 0.0
            ).astype(jnp.bfloat16)
        for c in tables:
            c.wait()
        terrain_load.wait()
        ew_lanes, sw_lanes = spread_table(ewt), spread_table(swt)
        firsts, seconds = [], []
        for c in range(tiles):
            tc = xi[0, :, c * LANE : (c + 1) * LANE]
            parts = [tc[i : i + SUB] for i in range(0, rows, SUB)]
            firsts.append(jnp.concatenate([pick(ew_lanes, x) for x in parts], axis=0))
            seconds.append(jnp.concatenate([pick(sw_lanes, x) for x in parts], axis=0))
        m = mb[...]
        mm = m * m
        mean_e, mean_s = block_means((firsts, seconds))
        own_f = mm / ((mm + half_point) * mean_e)
        own_q = m / mean_s
        fq[0] = own_f
        fq[1] = own_q
        for side in range(2):
            a, b = turn(own_f, SUB * side), turn(own_q, SUB * side + SUB)
            pk[side, 1] = jnp.where(lane < SUB, a, b)

        over((4, 5, 6, 7, 0, 1, 2, 3), lambda d: land_sends(d)[1].start())

        def valid(a, b):
            r = sub + (0 if a == 0 else jnp.where(upper, crow, -crow)) + gy * crow
            k = lane + (0 if b == 0 else jnp.where(left, ccol, -ccol)) + gx * ccol
            return (r >= 0) & (r < ny * crow) & (k >= 0) & (k < nx * ccol)

        ok = [[valid(a, b) for b in range(2)] for a in range(2)]
        over(range(8), lambda d: land_arrivals(d)[0].wait_recv())

        def joined(own, ns, k, g):
            ce = jnp.where(upper, pr[SE, k], pr[NE, k])
            cw = jnp.where(upper, pr[SW, k], pr[NW, k])
            t = [[own, unpack(pr[E, k], pr[W, k], g)], [ns, unpack(ce, cw, g)]]
            return [[jnp.where(ok[a][b], t[a][b], 0.0) for b in range(2)] for a in range(2)]

        def smooth(t):
            new = [[None, None], [None, None]]
            down = [[pltpu.roll(t[a][b], 1, 0) for b in range(2)] for a in range(2)]
            up = [[pltpu.roll(t[a][b], SUB - 1, 0) for b in range(2)] for a in range(2)]
            right = [[pltpu.roll(t[a][b], 1, 1) for b in range(2)] for a in range(2)]
            lft = [[pltpu.roll(t[a][b], LANE - 1, 1) for b in range(2)] for a in range(2)]
            for a in range(2):
                for b in range(2):
                    around = (
                        jnp.where(sub == 0, down[1 - a][b], down[a][b])
                        + jnp.where(sub == SUB - 1, up[1 - a][b], up[a][b])
                        + jnp.where(lane == 0, right[a][1 - b], right[a][b])
                        + jnp.where(lane == LANE - 1, lft[a][1 - b], lft[a][b])
                    )
                    value = t[a][b] + diffusion_rate * (around - 4.0 * t[a][b])
                    new[a][b] = jnp.where(ok[a][b], value, 0.0)
            return new

        precip = [[0.0, 0.0], [0.0, 0.0]]
        ground = None
        for l in range(lev):
            n, s = wr[N, l // 2], wr[S, l // 2]
            if l % 2 == 0:
                n = pltpu.roll(n, SUB // 2, 0)
            else:
                s = pltpu.roll(s, SUB // 2, 0)
            t = joined(wb[l], jnp.where(upper, s, n), 0, l)
            for _ in range(SWEEPS):
                t = smooth(t)
            if l == 0:
                ground = t[0][0]
            for a in range(2):
                for b in range(2):
                    precip[a][b] = precip[a][b] + lw[l] * t[a][b] * t[a][b]

        def ends(t):
            edge = jnp.where(
                left, jnp.broadcast_to(t[1][:, :1], (SUB, LANE)),
                jnp.broadcast_to(t[1][:, LANE - 1 :], (SUB, LANE)),
            )
            return [t[0], edge]

        over(range(8), lambda d: land_arrivals(d)[1].wait_recv())
        ratio = [
            joined(fq[f], jnp.where(upper, fr[S, f], fr[N, f]), 1, f) for f in range(2)
        ]
        for b, v in enumerate(ends(ratio[1][0])):
            qb[1, 0, :SUB, b * LANE : (b + 1) * LANE] = v
        s_send.start()
        own, ring = [
            ends([precip[a][b] * ratio[0][a][b] for b in range(2)]) for a in range(2)
        ]
        for b, v in enumerate(ends(ratio[1][1])):
            cs = slice(b * LANE, (b + 1) * LANE)
            qb[0, 0, :SUB, cs] = own[b]
            v = jnp.where(sub == 1, pltpu.roll(v, 1, 0), pltpu.roll(v, SUB - 1, 0))
            qb[0, 0, SUB:, cs] = jnp.where((sub == 1) | (sub == SUB - 2), v, ring[b])
        e_send.start()
        divisor = 1.0 + evaporation_scale * ground * ground
        over(range(8), lambda d: [c.wait_send() for c in land_sends(d)])
        s_send.wait_send()
        e_send.wait_send()
        back_send.wait_recv()
        out_ref[0] = back_rx[...] / divisor

    @pl.when(group == 1)
    def _():
        at_c = (iota((2 * SUB, LANE), 1) * AGG - iota((2 * SUB, LANE), 0)).astype(jnp.int16)
        one, none = jnp.ones((2 * SUB, LANE), jnp.bfloat16), jnp.zeros((2 * SUB, LANE), jnp.bfloat16)

        def place(k, at):
            j = pl.multiple_of(k * 2 * SUB, 2 * SUB)
            for c in range(tiles):
                perm[pl.ds(j, 2 * SUB), c * LANE : (c + 1) * LANE] = jnp.where(
                    at == jnp.int16(-c), one, none
                )
            return at - jnp.int16(2 * SUB)

        lax.fori_loop(0, cols // (2 * SUB), place, at_c, unroll=4)
        zero = jnp.zeros((SUB, LANE), jnp.float32)
        for c in range(width):
            for edge in (0, (bands + 1) * SUB):
                for k in (R, M0, M1):
                    st[k, c, edge : edge + SUB] = zero
                for k in (U, Q):
                    for p in range(2):
                        us[p, k, c, edge : edge + SUB] = zero

        for c in edges:
            c.wait()

        def stage(keff, code, head, tc):
            mixed = (code + 4 * tc).astype(jnp.float32).astype(jnp.bfloat16)
            return [mixed, *halves(keff), *halves(head)]

        def unmix(v, m, k, cs):
            got = [v[p * m + k : p * m + k + SUB, cs] for p in range(PLANES)]
            mixed = got[0].astype(jnp.int32)
            return got[1] + got[2], mixed & 3, got[3] + got[4], mixed >> 2

        chunk = 2 * LANE
        def both(ref, *lead):
            return jnp.concatenate([ref[(*lead, slice(e, e + SUB))] for e in ends], axis=0)

        edge = jnp.concatenate(
            stage(both(xf, 0) * both(act).astype(jnp.float32), both(xi, 1), both(xf, 1), both(xi, 0)),
            axis=0,
        )
        for n in range(0, cols, chunk):
            v = jnp.dot(edge, perm[:, n : n + chunk], preferred_element_type=jnp.float32)
            for c in range(n // LANE, (n + chunk) // LANE):
                cs = slice(c * LANE - n, c * LANE - n + LANE)
                for d in (N, S):
                    for f, x in enumerate(unmix(v, 2 * SUB, d * SUB, cs)):
                        hs[d, f, c] = x.astype(jnp.float32)

        pl.semaphore_wait(barrier, greeted)
        over((0, 1), lambda d: [c.start() for c in route_sends(d)])
        for c in rest:
            c.wait()
        order = [0, own_bands - 1] + list(range(1, own_bands - 1))
        for side in range(2):
            cs = slice(0, LANE) if side == 0 else slice(cols - LANE, cols)
            for q in range(sp.shape[1]):
                tile = zero
                for i, b in enumerate(order[4 * q : 4 * q + 4]):
                    o = slice(b * SUB, b * SUB + SUB)
                    keff = xf[0, o, cs] * act[o, cs].astype(jnp.float32)
                    values = (
                        keff, xi[1, o, cs].astype(jnp.float32), xf[1, o, cs],
                        xi[0, o, cs].astype(jnp.float32),
                    )
                    for f, v in enumerate(values):
                        g = i * FIELDS + f
                        tile = jnp.where(
                            (lane >= SUB * g) & (lane < SUB * g + SUB),
                            turn(v, SUB * g + SUB * side), tile,
                        )
                sp[side, q] = tile

        over((2, 3), lambda d: [c.start() for c in route_sends(d)])
        for c in tables:
            c.wait()
        ew_lanes, sw_lanes = spread_table(ewt), spread_table(swt)

        def put(c, o, keff, head, code, tc):
            live = keff > 0.0
            rs = lax.rsqrt(jnp.where(live, keff, 1.0))
            r = keff * rs
            rate = jnp.where(live, drainage_rate * infiltration_rate, 0.0)
            st[R, c, o] = r
            st[K, c, o] = keff
            st[RI, c, o] = jnp.where(live, rs * (1.0 / infiltration_rate), 0.0)
            st[AD, c, o] = rate
            st[M0, c, o] = jnp.where(code == 0, rate, 0.0)
            st[M1, c, o] = jnp.where(code == 1, rate, 0.0)
            st[M2, c, o] = jnp.where(code == 2, rate, jnp.where(code == 3, -rate, 0.0))
            st[EW, c, o] = r * pick(ew_lanes, tc)
            st[HD, c, o] = r * head
            st[SO, c, o] = pick(sw_lanes, tc) * (1.0 / infiltration_rate)

        def aligned(x):
            return x if isinstance(x, int) else pl.multiple_of(x, SUB)

        middle = rows - 2 * SUB
        for i in range(0, middle, 2 * SUB):
            o = slice(SUB + i, 3 * SUB + i)
            parts = stage(xf[0, o] * act[o].astype(jnp.float32), xi[1, o], xf[1, o], xi[0, o])
            for p, x in enumerate(parts):
                planes[p * middle + i : p * middle + i + 2 * SUB, :] = x
        for n in range(0, cols, chunk):
            v = jnp.dot(planes[...], perm[:, n : n + chunk], preferred_element_type=jnp.float32)
            for c in range(n // LANE, (n + chunk) // LANE):
                cs = slice(c * LANE - n, c * LANE - n + LANE)
                for t in range(2, bands - 2):
                    keff, code, head, tc = unmix(v, middle, (t - 2) * SUB, cs)
                    put(c, slice(t * SUB + SUB, t * SUB + 2 * SUB), keff, head, code, tc)

        def put_row(t, ref, d, there):
            for c in range(tiles):
                keff, code, head, tc = [
                    jnp.where((lane >= 0) & there, ref[d, f, c], 0.0) for f in range(FIELDS)
                ]
                put(c, slice(t * SUB + SUB, t * SUB + 2 * SUB), keff, head, code,
                    tc.astype(jnp.int32))

        yes = gy >= 0
        put_row(1, hs, N, yes)
        put_row(bands - 2, hs, S, yes)

        over((W, E), lambda d: [c.wait_recv() for c in route_arrivals(d)])
        corners(lambda d, s: corner_send(d, s).start())

        def side_ok(there):
            reach = (lane < SUB) & exists(E) | (lane >= LANE - SUB) & exists(W)
            return reach & there

        def put_side(t, east, west, g, there):
            ok = side_ok(there)
            keff, code, head, tc = [unpack(east, west, g + f) for f in range(FIELDS)]
            put(
                tiles, slice(t * SUB + SUB, t * SUB + 2 * SUB), jnp.where(ok, keff, 0.0),
                jnp.where(ok, head, 0.0), jnp.where(ok, code, 0.0),
                jnp.where(ok, tc, 0.0).astype(jnp.int32),
            )

        for i, b in enumerate(order):
            put_side(b + 1, sr[1, i // 4], sr[0, i // 4], (i % 4) * FIELDS, yes)

        def beside(west_of, east_of):
            w, e = west_of, east_of
            last = tiles - 1
            w_end, w_side = pltpu.roll(w[last], 1, 1), pltpu.roll(w[tiles], 1, 1)
            e_end, e_side = pltpu.roll(e[0], LANE - 1, 1), pltpu.roll(e[tiles], LANE - 1, 1)
            first, final = lane == 0, lane == LANE - 1
            west = [jnp.where(first, w_side, w_end), *w[:last], jnp.where(first, w_end, w_side)]
            east = [*e[1:tiles], jnp.where(final, e_side, e_end), jnp.where(final, e_end, e_side)]
            return west, east

        def around(t):
            base = aligned(t * SUB + SUB)
            return pl.ds(base, SUB), pl.ds(base - 1, SUB), pl.ds(base + 1, SUB)

        def couple(t, carry):
            o, above, below = around(t)
            r = [st[R, c, o] for c in range(width)]
            west, east = beside(r, r)
            for c in range(width):
                total = (st[R, c, above] + st[R, c, below]) + (west[c] + east[c])
                st[A1, c, o] = 1.0 - r[c] * total
            return carry

        lax.fori_loop(2, bands - 2, couple, 0, unroll=2)

        over((N, S), lambda d: [c.wait_recv() for c in route_arrivals(d)])
        corners(lambda d, s: corner_arrival(d, s).wait_recv())
        for t, d, g in ((0, N, FIELDS), (bands - 1, S, 0)):
            put_row(t, hr, d, exists(d))
            put_side(t, cr[d, 1], cr[d, 0], g, exists(d))
        for t in (0, 1, bands - 2, bands - 1):
            couple(t, 0)

        def up(k, t):
            ring = 0 if t in (0, bands - 1) else k
            if t == 0:
                a = b = 2 * crow - 1 - k
            elif t == bands - 1:
                a = b = crow + k
            else:
                a, b = ((t - 1) * SUB) // AGG, ((t - 1) * SUB + SUB - 1) // AGG
            got = []
            for side in range(2):
                cs = slice(side * LANE, side * LANE + LANE)
                v = jnp.broadcast_to(qb[ring, 1, a : a + 1, cs], (SUB, LANE))
                if a != b:
                    second = jnp.broadcast_to(qb[ring, 1, b : b + 1, cs], (SUB, LANE))
                    v = jnp.where(sub < b * AGG - (t - 1) * SUB, v, second)
                got.append(v)
            return [got[0]] * tiles + [got[1]]

        def start_y(t):
            o = slice((t + 1) * SUB, (t + 2) * SUB)
            for c, v in enumerate(up(1, t)):
                y = st[SO, c, o] * v
                us[0, Y, c, o] = y
                us[0, Q, c, o] = y * y

        s_send.wait_recv()
        for t in range(1, bands - 1):
            start_y(t)

        e_send.wait_recv()
        start_y(0)
        start_y(bands - 1)
        for t in range(bands):
            o = slice((t + 1) * SUB, (t + 2) * SUB)
            for c, v in enumerate(up(0, t)):
                us[0, U, c, o] = st[HD, c, o] + st[EW, c, o] * v

        full = 1.0 / infiltration_rate

        def flows(q, o):
            h = [st[M2, c, o] * q[c] for c in range(width)]
            west, east = beside(h, h)
            return [
                jnp.maximum(east[c], 0.0) - jnp.minimum(west[c], 0.0) for c in range(width)
            ]

        def sums_u(u):
            west, east = beside(u, u)
            return [west[c] + east[c] for c in range(width)]

        def new_y(src, c, o, above, below, y, q, gu, side):
            return (
                (y + st[RI, c, o] * gu)
                + (st[M0, c, below] * us[src, Q, c, below] + st[M1, c, above] * us[src, Q, c, above])
                + (side - st[AD, c, o] * q)
            )

        def new_u(src, c, o, above, below, u, gu, side):
            total = (us[src, U, c, above] + us[src, U, c, below]) + side
            return (st[A1, c, o] * u - gu) + st[K, c, o] * total

        def held(src, k, o):
            return [us[src, k, c, o] for c in range(width)]

        def substep(src, dst):
            def band(t, carry):
                o, above, below = around(t)
                last = tiles - 1

                def get_u(c):
                    return us[src, U, c, o]

                def get_h(c):
                    return st[M2, c, o] * us[src, Q, c, o]

                ends = []
                for get in (get_u, get_h):
                    w_end, w_side = pltpu.roll(get(last), 1, 1), pltpu.roll(get(tiles), 1, 1)
                    e_end, e_side = (
                        pltpu.roll(get(0), LANE - 1, 1), pltpu.roll(get(tiles), LANE - 1, 1)
                    )
                    ends.append((w_end, w_side, e_end, e_side))
                first, final = lane == 0, lane == LANE - 1
                u, h = {}, {}
                for c in [*range(1, width), 0]:
                    for k in (c - 1, c, c + 1):
                        if k in range(width) and (c not in (0, tiles) or k == c) and k not in u:
                            u[k], h[k] = get_u(k), get_h(k)
                    west, east = [], []
                    for near, (w_end, w_side, e_end, e_side) in zip((u, h), ends):
                        if c == 0:
                            west.append(jnp.where(first, w_side, w_end))
                        elif c == tiles:
                            west.append(jnp.where(first, w_end, w_side))
                        else:
                            west.append(near[c - 1])
                        if c == last:
                            east.append(jnp.where(final, e_side, e_end))
                        elif c == tiles:
                            east.append(jnp.where(final, e_end, e_side))
                        else:
                            east.append(near[c + 1])
                    y = us[src, Y, c, o]
                    gu = u[c] * pl.reciprocal(y + full)
                    side = jnp.maximum(east[1], 0.0) - jnp.minimum(west[1], 0.0)
                    us[dst, U, c, o] = new_u(src, c, o, above, below, u[c], gu, west[0] + east[0])
                    y = new_y(src, c, o, above, below, y, us[src, Q, c, o], gu, side)
                    us[dst, Y, c, o] = y
                    us[dst, Q, c, o] = y * y
                return carry

            lax.fori_loop(0, bands, band, 0, unroll=UNROLL)

        def two(k, carry):
            substep(0, 1)
            substep(1, 0)
            return carry

        lax.fori_loop(0, NSUB // 2 - 1, two, 0)
        substep(0, 1)

        def last_y(t, carry):
            o, above, below = around(t)
            u, q = held(1, U, o), held(1, Q, o)
            q_sides = flows(q, o)
            total = None
            for c in range(tiles):
                y = us[1, Y, c, o]
                gu = u[c] * pl.reciprocal(y + full)
                y = new_y(1, c, o, above, below, y, q[c], gu, q_sides[c])
                total = y if total is None else total + y
            sums[0, pl.ds(aligned(t * SUB - SUB), SUB)] = total
            return carry

        def last_u(t, carry):
            o, above, below = around(t)
            u = held(1, U, o)
            u_sides = sums_u(u)
            total = None
            for c in range(tiles):
                gu = u[c] * pl.reciprocal(us[1, Y, c, o] + full)
                p = new_u(1, c, o, above, below, u[c], gu, u_sides[c]) * st[RI, c, o]
                total = p if total is None else total + p
            sums[1, pl.ds(aligned(t * SUB - SUB), SUB)] = total
            return carry

        lax.fori_loop(1, bands - 1, last_y, 0, unroll=True)
        back_tx[...] = pool(sums[0], infiltration_rate)
        back_send.start()
        lax.fori_loop(1, bands - 1, last_u, 0, unroll=True)
        out_ref[0] = pool(sums[1], infiltration_rate)
        over(range(4), lambda d: [c.wait_send() for c in route_sends(d)])
        corners(lambda d, s: corner_send(d, s).wait_send())
        back_send.wait_send()


UNROLL = 12


def per_device(ny, nx, column_water, land_soil, level_weight, excess_weight, soil_weight,
               terrain_class, surface_head, conductivity, active_mask, flow_code):
    rows, cols = terrain_class.shape
    lev = column_water.shape[1]
    crow, ccol = land_soil.shape[1:]
    wide = cols // LANE + 1
    tall = rows + 4 * SUB
    packs = -(-(rows // SUB) // 4)
    f32, i32, bf16 = jnp.float32, jnp.int32, jnp.bfloat16
    hbm = pl.BlockSpec(memory_space=pltpu.HBM)
    return pl.pallas_call(
        functools.partial(kernel, ny, nx),
        out_shape=pltpu.VMEM((1, crow, ccol), f32),
        in_specs=[hbm] * 10,
        out_specs=pl.BlockSpec(memory_space=pltpu.VMEM),
        scratch_shapes=[
            pltpu.SMEM(level_weight.shape, f32),
            pltpu.SMEM(excess_weight.shape, f32),
            pltpu.SMEM(soil_weight.shape, f32),
            pltpu.VMEM((2, rows, cols), i32),
            pltpu.VMEM((rows, cols), i32),
            pltpu.VMEM((2, rows, cols), f32),
            pltpu.VMEM((11, wide, tall, LANE), f32),
            pltpu.VMEM((2, 3, wide, tall, LANE), f32),
            pltpu.VMEM((lev, crow, ccol), f32),
            pltpu.VMEM((crow, ccol), f32),
            pltpu.VMEM((2, lev // 2, crow, ccol), f32),
            pltpu.VMEM((2, lev // 2, crow, ccol), f32),
            pltpu.VMEM((2, 2, crow, ccol), f32),
            pltpu.VMEM((8, 2, crow, ccol), f32),
            pltpu.VMEM((2, crow, ccol), f32),
            pltpu.VMEM((2, 2, crow, ccol), f32),
            pltpu.VMEM((2, 2, 2 * crow, 2 * ccol), f32),
            pltpu.VMEM((crow, ccol), f32),
            pltpu.VMEM((crow, ccol), f32),
            pltpu.VMEM((cols, ccol), bf16),
            pltpu.VMEM((cols, cols), bf16),
            pltpu.VMEM((PLANES * (rows - 2 * SUB), cols), bf16),
            pltpu.VMEM((2, FIELDS, wide - 1, SUB, LANE), f32),
            pltpu.VMEM((2, FIELDS, wide - 1, SUB, LANE), f32),
            pltpu.VMEM((2, rows, LANE), f32),
            pltpu.VMEM((2, packs, SUB, LANE), f32),
            pltpu.VMEM((2, packs, SUB, LANE), f32),
            pltpu.VMEM((2, 2, SUB, LANE), f32),
            pltpu.SemaphoreType.DMA((8, 3)),
            pltpu.SemaphoreType.DMA((8, 3)),
            pltpu.SemaphoreType.DMA((18,)),
            pltpu.SemaphoreType.DMA((6,)),
        ],
        compiler_params=pltpu.CompilerParams(
            collective_id=0, has_side_effects=True
        ),
    )(level_weight, excess_weight, soil_weight, column_water, land_soil, terrain_class,
      surface_head, conductivity, active_mask, flow_code)


def solution(mesh):
    in_specs = (
        P("comp", None, "gy", "gx"),
        P("comp", "gy", "gx"),
        P(),
        P(),
        P(),
        P("gy", "gx"),
        P("comp", "gy", "gx"),
        P("comp", "gy", "gx"),
        P("comp", "gy", "gx"),
        P("comp", "gy", "gx"),
    )
    body = functools.partial(per_device, mesh.shape["gy"], mesh.shape["gx"])
    return jax.shard_map(
        body, mesh=mesh, in_specs=in_specs, out_specs=P("comp", "gy", "gx"), check_vma=False
    )
```

```python
import functools

import jax
import jax.numpy as jnp
from jax import lax
from jax.experimental import pallas as pl
from jax.experimental.pallas import tpu as pltpu
from jax.sharding import PartitionSpec as P

AGG = 10
NSUB = 8
SWEEPS = 2

diffusion_rate = 0.2
infiltration_rate = 0.05
drainage_rate = 0.1
half_point = 0.1
evaporation_scale = 0.5

LANE = 128
SUB = 8
MESH = pl.DeviceIdType.MESH
DIRS = ((-1, 0), (1, 0), (0, -1), (0, 1), (-1, -1), (-1, 1), (1, -1), (1, 1))
N, S, W, E, NW, NE, SW, SE = range(8)
OPP = (S, N, E, W, SE, SW, NE, NW)

R, K, RI, AD, M0, M1, M2, EW, HD, SO, A1 = range(11)
PLANES = 5
U, Y, Q = range(3)
FIELDS = 4


def iota(shape, dim):
    return lax.broadcasted_iota(jnp.int32, shape, dim)


def pick(lanes, classes):
    return jnp.take_along_axis(lanes, classes, axis=1, mode="promise_in_bounds")


def halves(x):
    high = x.astype(jnp.bfloat16)
    return high, (x - high.astype(jnp.float32)).astype(jnp.bfloat16)


def turn(x, shift):
    shift %= LANE
    return pltpu.roll(x, shift, 1) if shift else x


def kernel(
    ny, nx,
    lw_in, ewt_in, swt_in, water_in, soil_in, terrain_in, head_in, cond_in, active_in, code_in,
    out_ref,
    lw, ewt, swt, xi, act, xf, st, us, wb, mb, wp, wr, pk, pr, fq, fr, qb, back_tx, back_rx,
    gather, perm, planes, hs, hr, sums, sp, sr, cr, send, recv, local, hop,
):
    group = lax.axis_index("comp")
    gy = lax.axis_index("gy")
    gx = lax.axis_index("gx")
    rows, cols = terrain_in.shape
    lev = water_in.shape[1]
    crow, ccol = soil_in.shape[1], soil_in.shape[2]
    tiles = cols // LANE
    width = tiles + 1
    own_bands = rows // SUB
    bands = own_bands + 2

    lane = iota((SUB, LANE), 1)
    sub = iota((SUB, LANE), 0)
    left = lane < LANE // 2
    upper = sub < SUB // 2

    def exists(d):
        dy, dx = DIRS[d]
        return (gy + dy >= 0) & (gy + dy < ny) & (gx + dx >= 0) & (gx + dx < nx)

    def at(d):
        dy, dx = DIRS[d]
        return {"comp": group, "gy": gy + dy, "gx": gx + dx}

    partner = {"comp": 1 - group, "gy": gy, "gx": gx}

    def copy(src, dst, d, f):
        return pltpu.make_async_remote_copy(
            src_ref=src, dst_ref=dst, send_sem=send.at[d, f], recv_sem=recv.at[OPP[d], f],
            device_id=at(d), device_id_type=MESH,
        )

    def arrival(dst, d, f):
        return pltpu.make_async_remote_copy(
            src_ref=dst, dst_ref=dst, send_sem=send.at[d, f], recv_sem=recv.at[d, f],
            device_id=at(d), device_id_type=MESH,
        )

    def across(src, dst, k):
        return pltpu.make_async_remote_copy(
            src_ref=src, dst_ref=dst, send_sem=hop.at[2 * k], recv_sem=hop.at[2 * k + 1],
            device_id=partner, device_id_type=MESH,
        )

    def spread_table(table):
        v = jnp.zeros((SUB, LANE), jnp.float32)
        for k in range(table.shape[0]):
            v = jnp.where(lane == k, table[k], v)
        return v

    def over(dirs, action):
        for d in dirs:
            @pl.when(exists(d))
            def _():
                action(d)

    def load(src, dst, k):
        return pltpu.make_async_copy(src, dst, local.at[k])

    tables = [load(a, b, k) for k, (a, b) in enumerate(((lw_in, lw), (ewt_in, ewt), (swt_in, swt)))]
    terrain_load = load(terrain_in, xi.at[0], 3)
    land_loads = [load(water_in.at[0], wb, 4), load(soil_in.at[0], mb, 5)]
    ends = (0, rows - SUB)
    bulk = [
        (cond_in.at[0], xf.at[0]), (active_in.at[0], act), (code_in.at[0], xi.at[1]),
        (head_in.at[0], xf.at[1]), (terrain_in, xi.at[0]),
    ]

    def some(refs, start, size, k):
        return load(*[r.at[pl.ds(start, size)] for r in refs], k)

    edges = [some(r, e, SUB, 3 + 2 * k + i) for k, r in enumerate(bulk) for i, e in enumerate(ends)]
    rest = [some(r, SUB, rows - 2 * SUB, 13 + k) for k, r in enumerate(bulk)]

    barrier = pltpu.get_barrier_semaphore()
    greeted = 1
    for d in range(8):
        meet = exists(d) if d < 4 else exists(d) & (group == 0)
        greeted = greeted + meet.astype(jnp.int32)

        @pl.when(meet)
        def _():
            pl.semaphore_signal(barrier, inc=1, device_id=at(d), device_id_type=MESH)
    pl.semaphore_signal(barrier, inc=1, device_id=partner, device_id_type=MESH)

    @pl.when(group == 0)
    def _():
        for c in land_loads:
            c.start()
        terrain_load.start()

    @pl.when(group == 1)
    def _():
        for c in edges + rest:
            c.start()

    for c in tables:
        c.start()

    def land_sends(d):
        if d < 2:
            return [copy(wp.at[d], wr.at[OPP[d]], d, 0), copy(fq, fr.at[OPP[d]], d, 1)]
        side = 0 if DIRS[d][1] < 0 else 1
        return [copy(pk.at[side, k], pr.at[OPP[d], k], d, k) for k in range(2)]

    def land_arrivals(d):
        if d < 2:
            return [arrival(wr.at[d], d, 0), arrival(fr.at[d], d, 1)]
        return [arrival(pr.at[d, k], d, k) for k in range(2)]

    def route_sends(d):
        if d < 2:
            return [copy(hs.at[d], hr.at[OPP[d]], d, 0)]
        return [copy(sp.at[d - 2], sr.at[OPP[d] - 2], d, 0)]

    def route_arrivals(d):
        return [arrival(hr.at[d] if d < 2 else sr.at[d - 2], d, 0)]

    def corner_send(d, s):
        return copy(sr.at[s, 0], cr.at[OPP[d], s], d, 1 + s)

    def corner_arrival(d, s):
        return arrival(cr.at[d, s], d, 1 + s)

    def corners(action):
        for d in (N, S):
            for s in (0, 1):
                @pl.when(exists(d) & exists(W + s))
                def _():
                    action(d, s)

    s_send = across(qb.at[1, 0, pl.ds(0, SUB)], qb.at[1, 1, pl.ds(0, SUB)], 0)
    e_send = across(qb.at[0, 0], qb.at[0, 1], 1)
    back_send = across(back_tx, back_rx, 2)

    def pool_rows():
        i10 = iota((crow, rows), 0) * AGG
        i = iota((crow, rows), 1)
        ones = jnp.where((i >= i10) & (i < i10 + AGG), 1.0, 0.0).astype(jnp.bfloat16)
        return jnp.concatenate([ones, ones], axis=1)

    def pool(z, scale):
        return jnp.dot(
            pool_rows(), jnp.concatenate(halves(z), axis=0), preferred_element_type=jnp.float32
        ) * (scale / (AGG * AGG))

    def block_means(fields):
        ones = pool_rows()
        summed = []
        for field in fields:
            parts = [jnp.concatenate(halves(tile), axis=0) for tile in field]
            summed.append(
                jnp.dot(ones, jnp.concatenate(parts, axis=1), preferred_element_type=jnp.float32)
            )
        stacked = jnp.concatenate(halves(jnp.concatenate(summed, axis=0)), axis=0)
        y = jnp.dot(stacked, gather[...], preferred_element_type=jnp.float32)
        total = (y[: 2 * crow] + y[2 * crow :]) * (1.0 / (AGG * AGG))
        return total[:crow], total[crow:]

    def unpack(east, west, g):
        return jnp.where(left, turn(east, -SUB * g), turn(west, -SUB * g - SUB))

    @pl.when(group == 0)
    def _():
        for c in land_loads:
            c.wait()
        packs = [jnp.zeros((SUB, LANE), jnp.float32)] * 2
        for l in range(lev):
            mine = (lane >= SUB * l) & (lane < SUB * l + SUB)
            w = wb[l]
            packs[0] = jnp.where(mine, turn(w, SUB * l), packs[0])
            packs[1] = jnp.where(mine, turn(w, SUB * l + SUB), packs[1])
        pk[0, 0] = packs[0]
        pk[1, 0] = packs[1]
        for i in range(lev // 2):
            a, b = wb[2 * i], wb[2 * i + 1]
            wp[N, i] = jnp.where(upper, a, pltpu.roll(b, SUB // 2, 0))
            wp[S, i] = jnp.where(upper, pltpu.roll(a, SUB // 2, 0), b)

        pl.semaphore_wait(barrier, greeted)
        over((4, 5, 6, 7, 0, 1, 2, 3), lambda d: land_sends(d)[0].start())

        k10 = iota((LANE, ccol), 1) * AGG
        j0 = iota((LANE, ccol), 0)
        for c in range(tiles):
            j = j0 + c * LANE
            gather[c * LANE : (c + 1) * LANE, :] = jnp.where(
                (j >= k10) & (j < k10 + AGG), 1.0, 0.0
            ).astype(jnp.bfloat16)
        for c in tables:
            c.wait()
        terrain_load.wait()
        ew_lanes, sw_lanes = spread_table(ewt), spread_table(swt)
        firsts, seconds = [], []
        for c in range(tiles):
            tc = xi[0, :, c * LANE : (c + 1) * LANE]
            parts = [tc[i : i + SUB] for i in range(0, rows, SUB)]
            firsts.append(jnp.concatenate([pick(ew_lanes, x) for x in parts], axis=0))
            seconds.append(jnp.concatenate([pick(sw_lanes, x) for x in parts], axis=0))
        m = mb[...]
        mm = m * m
        mean_e, mean_s = block_means((firsts, seconds))
        own_f = mm / ((mm + half_point) * mean_e)
        own_q = m / mean_s
        fq[0] = own_f
        fq[1] = own_q
        for side in range(2):
            a, b = turn(own_f, SUB * side), turn(own_q, SUB * side + SUB)
            pk[side, 1] = jnp.where(lane < SUB, a, b)

        over((4, 5, 6, 7, 0, 1, 2, 3), lambda d: land_sends(d)[1].start())

        def valid(a, b):
            r = sub + (0 if a == 0 else jnp.where(upper, crow, -crow)) + gy * crow
            k = lane + (0 if b == 0 else jnp.where(left, ccol, -ccol)) + gx * ccol
            return (r >= 0) & (r < ny * crow) & (k >= 0) & (k < nx * ccol)

        ok = [[valid(a, b) for b in range(2)] for a in range(2)]
        over(range(8), lambda d: land_arrivals(d)[0].wait_recv())

        def joined(own, ns, k, g):
            ce = jnp.where(upper, pr[SE, k], pr[NE, k])
            cw = jnp.where(upper, pr[SW, k], pr[NW, k])
            t = [[own, unpack(pr[E, k], pr[W, k], g)], [ns, unpack(ce, cw, g)]]
            return [[jnp.where(ok[a][b], t[a][b], 0.0) for b in range(2)] for a in range(2)]

        def smooth(t):
            new = [[None, None], [None, None]]
            down = [[pltpu.roll(t[a][b], 1, 0) for b in range(2)] for a in range(2)]
            up = [[pltpu.roll(t[a][b], SUB - 1, 0) for b in range(2)] for a in range(2)]
            right = [[pltpu.roll(t[a][b], 1, 1) for b in range(2)] for a in range(2)]
            lft = [[pltpu.roll(t[a][b], LANE - 1, 1) for b in range(2)] for a in range(2)]
            for a in range(2):
                for b in range(2):
                    around = (
                        jnp.where(sub == 0, down[1 - a][b], down[a][b])
                        + jnp.where(sub == SUB - 1, up[1 - a][b], up[a][b])
                        + jnp.where(lane == 0, right[a][1 - b], right[a][b])
                        + jnp.where(lane == LANE - 1, lft[a][1 - b], lft[a][b])
                    )
                    value = t[a][b] + diffusion_rate * (around - 4.0 * t[a][b])
                    new[a][b] = jnp.where(ok[a][b], value, 0.0)
            return new

        precip = [[0.0, 0.0], [0.0, 0.0]]
        ground = None
        for l in range(lev):
            n, s = wr[N, l // 2], wr[S, l // 2]
            if l % 2 == 0:
                n = pltpu.roll(n, SUB // 2, 0)
            else:
                s = pltpu.roll(s, SUB // 2, 0)
            t = joined(wb[l], jnp.where(upper, s, n), 0, l)
            for _ in range(SWEEPS):
                t = smooth(t)
            if l == 0:
                ground = t[0][0]
            for a in range(2):
                for b in range(2):
                    precip[a][b] = precip[a][b] + lw[l] * t[a][b] * t[a][b]

        def ends(t):
            edge = jnp.where(
                left, jnp.broadcast_to(t[1][:, :1], (SUB, LANE)),
                jnp.broadcast_to(t[1][:, LANE - 1 :], (SUB, LANE)),
            )
            return [t[0], edge]

        over(range(8), lambda d: land_arrivals(d)[1].wait_recv())
        ratio = [
            joined(fq[f], jnp.where(upper, fr[S, f], fr[N, f]), 1, f) for f in range(2)
        ]
        for b, v in enumerate(ends(ratio[1][0])):
            qb[1, 0, :SUB, b * LANE : (b + 1) * LANE] = v
        s_send.start()
        own, ring = [
            ends([precip[a][b] * ratio[0][a][b] for b in range(2)]) for a in range(2)
        ]
        for b, v in enumerate(ends(ratio[1][1])):
            cs = slice(b * LANE, (b + 1) * LANE)
            qb[0, 0, :SUB, cs] = own[b]
            v = jnp.where(sub == 1, pltpu.roll(v, 1, 0), pltpu.roll(v, SUB - 1, 0))
            qb[0, 0, SUB:, cs] = jnp.where((sub == 1) | (sub == SUB - 2), v, ring[b])
        e_send.start()
        divisor = 1.0 + evaporation_scale * ground * ground
        over(range(8), lambda d: [c.wait_send() for c in land_sends(d)])
        s_send.wait_send()
        e_send.wait_send()
        back_send.wait_recv()
        out_ref[0] = back_rx[...] / divisor

    @pl.when(group == 1)
    def _():
        at_c = (iota((2 * SUB, LANE), 1) * AGG - iota((2 * SUB, LANE), 0)).astype(jnp.int16)
        one, none = jnp.ones((2 * SUB, LANE), jnp.bfloat16), jnp.zeros((2 * SUB, LANE), jnp.bfloat16)

        def place(k, at):
            j = pl.multiple_of(k * 2 * SUB, 2 * SUB)
            for c in range(tiles):
                perm[pl.ds(j, 2 * SUB), c * LANE : (c + 1) * LANE] = jnp.where(
                    at == jnp.int16(-c), one, none
                )
            return at - jnp.int16(2 * SUB)

        lax.fori_loop(0, cols // (2 * SUB), place, at_c, unroll=4)
        zero = jnp.zeros((SUB, LANE), jnp.float32)
        for c in range(width):
            for edge in (0, (bands + 1) * SUB):
                for k in (R, M0, M1):
                    st[k, c, edge : edge + SUB] = zero
                for k in (U, Q):
                    for p in range(2):
                        us[p, k, c, edge : edge + SUB] = zero

        for c in edges:
            c.wait()

        def stage(keff, code, head, tc):
            mixed = (code + 4 * tc).astype(jnp.float32).astype(jnp.bfloat16)
            return [mixed, *halves(keff), *halves(head)]

        def unmix(v, m, k, cs):
            got = [v[p * m + k : p * m + k + SUB, cs] for p in range(PLANES)]
            mixed = got[0].astype(jnp.int32)
            return got[1] + got[2], mixed & 3, got[3] + got[4], mixed >> 2

        chunk = 2 * LANE
        def both(ref, *lead):
            return jnp.concatenate([ref[(*lead, slice(e, e + SUB))] for e in ends], axis=0)

        edge = jnp.concatenate(
            stage(both(xf, 0) * both(act).astype(jnp.float32), both(xi, 1), both(xf, 1), both(xi, 0)),
            axis=0,
        )
        for n in range(0, cols, chunk):
            v = jnp.dot(edge, perm[:, n : n + chunk], preferred_element_type=jnp.float32)
            for c in range(n // LANE, (n + chunk) // LANE):
                cs = slice(c * LANE - n, c * LANE - n + LANE)
                for d in (N, S):
                    for f, x in enumerate(unmix(v, 2 * SUB, d * SUB, cs)):
                        hs[d, f, c] = x.astype(jnp.float32)

        pl.semaphore_wait(barrier, greeted)
        over((0, 1), lambda d: [c.start() for c in route_sends(d)])
        for c in rest:
            c.wait()
        order = [0, own_bands - 1] + list(range(1, own_bands - 1))
        for side in range(2):
            cs = slice(0, LANE) if side == 0 else slice(cols - LANE, cols)
            for q in range(sp.shape[1]):
                tile = zero
                for i, b in enumerate(order[4 * q : 4 * q + 4]):
                    o = slice(b * SUB, b * SUB + SUB)
                    keff = xf[0, o, cs] * act[o, cs].astype(jnp.float32)
                    values = (
                        keff, xi[1, o, cs].astype(jnp.float32), xf[1, o, cs],
                        xi[0, o, cs].astype(jnp.float32),
                    )
                    for f, v in enumerate(values):
                        g = i * FIELDS + f
                        tile = jnp.where(
                            (lane >= SUB * g) & (lane < SUB * g + SUB),
                            turn(v, SUB * g + SUB * side), tile,
                        )
                sp[side, q] = tile

        over((2, 3), lambda d: [c.start() for c in route_sends(d)])
        for c in tables:
            c.wait()
        ew_lanes, sw_lanes = spread_table(ewt), spread_table(swt)

        def put(c, o, keff, head, code, tc):
            live = keff > 0.0
            rs = lax.rsqrt(jnp.where(live, keff, 1.0))
            r = keff * rs
            rate = jnp.where(live, drainage_rate * infiltration_rate, 0.0)
            st[R, c, o] = r
            st[K, c, o] = keff
            st[RI, c, o] = jnp.where(live, rs * (1.0 / infiltration_rate), 0.0)
            st[AD, c, o] = rate
            st[M0, c, o] = jnp.where(code == 0, rate, 0.0)
            st[M1, c, o] = jnp.where(code == 1, rate, 0.0)
            st[M2, c, o] = jnp.where(code == 2, rate, jnp.where(code == 3, -rate, 0.0))
            st[EW, c, o] = r * pick(ew_lanes, tc)
            st[HD, c, o] = r * head
            st[SO, c, o] = pick(sw_lanes, tc) * (1.0 / infiltration_rate)

        def aligned(x):
            return x if isinstance(x, int) else pl.multiple_of(x, SUB)

        middle = rows - 2 * SUB
        for i in range(0, middle, 2 * SUB):
            o = slice(SUB + i, 3 * SUB + i)
            parts = stage(xf[0, o] * act[o].astype(jnp.float32), xi[1, o], xf[1, o], xi[0, o])
            for p, x in enumerate(parts):
                planes[p * middle + i : p * middle + i + 2 * SUB, :] = x
        for n in range(0, cols, chunk):
            v = jnp.dot(planes[...], perm[:, n : n + chunk], preferred_element_type=jnp.float32)
            for c in range(n // LANE, (n + chunk) // LANE):
                cs = slice(c * LANE - n, c * LANE - n + LANE)
                for t in range(2, bands - 2):
                    keff, code, head, tc = unmix(v, middle, (t - 2) * SUB, cs)
                    put(c, slice(t * SUB + SUB, t * SUB + 2 * SUB), keff, head, code, tc)

        def put_row(t, ref, d, there):
            for c in range(tiles):
                keff, code, head, tc = [
                    jnp.where((lane >= 0) & there, ref[d, f, c], 0.0) for f in range(FIELDS)
                ]
                put(c, slice(t * SUB + SUB, t * SUB + 2 * SUB), keff, head, code,
                    tc.astype(jnp.int32))

        yes = gy >= 0
        put_row(1, hs, N, yes)
        put_row(bands - 2, hs, S, yes)

        over((W, E), lambda d: [c.wait_recv() for c in route_arrivals(d)])
        corners(lambda d, s: corner_send(d, s).start())

        def side_ok(there):
            reach = (lane < SUB) & exists(E) | (lane >= LANE - SUB) & exists(W)
            return reach & there

        def put_side(t, east, west, g, there):
            ok = side_ok(there)
            keff, code, head, tc = [unpack(east, west, g + f) for f in range(FIELDS)]
            put(
                tiles, slice(t * SUB + SUB, t * SUB + 2 * SUB), jnp.where(ok, keff, 0.0),
                jnp.where(ok, head, 0.0), jnp.where(ok, code, 0.0),
                jnp.where(ok, tc, 0.0).astype(jnp.int32),
            )

        for i, b in enumerate(order):
            put_side(b + 1, sr[1, i // 4], sr[0, i // 4], (i % 4) * FIELDS, yes)

        def beside(west_of, east_of):
            w, e = west_of, east_of
            last = tiles - 1
            w_end, w_side = pltpu.roll(w[last], 1, 1), pltpu.roll(w[tiles], 1, 1)
            e_end, e_side = pltpu.roll(e[0], LANE - 1, 1), pltpu.roll(e[tiles], LANE - 1, 1)
            first, final = lane == 0, lane == LANE - 1
            west = [jnp.where(first, w_side, w_end), *w[:last], jnp.where(first, w_end, w_side)]
            east = [*e[1:tiles], jnp.where(final, e_side, e_end), jnp.where(final, e_end, e_side)]
            return west, east

        def around(t):
            base = aligned(t * SUB + SUB)
            return pl.ds(base, SUB), pl.ds(base - 1, SUB), pl.ds(base + 1, SUB)

        def couple(t, carry):
            o, above, below = around(t)
            r = [st[R, c, o] for c in range(width)]
            west, east = beside(r, r)
            for c in range(width):
                total = (st[R, c, above] + st[R, c, below]) + (west[c] + east[c])
                st[A1, c, o] = 1.0 - r[c] * total
            return carry

        lax.fori_loop(2, bands - 2, couple, 0, unroll=2)

        over((N, S), lambda d: [c.wait_recv() for c in route_arrivals(d)])
        corners(lambda d, s: corner_arrival(d, s).wait_recv())
        for t, d, g in ((0, N, FIELDS), (bands - 1, S, 0)):
            put_row(t, hr, d, exists(d))
            put_side(t, cr[d, 1], cr[d, 0], g, exists(d))
        for t in (0, 1, bands - 2, bands - 1):
            couple(t, 0)

        def up(k, t):
            ring = 0 if t in (0, bands - 1) else k
            if t == 0:
                a = b = 2 * crow - 1 - k
            elif t == bands - 1:
                a = b = crow + k
            else:
                a, b = ((t - 1) * SUB) // AGG, ((t - 1) * SUB + SUB - 1) // AGG
            got = []
            for side in range(2):
                cs = slice(side * LANE, side * LANE + LANE)
                v = jnp.broadcast_to(qb[ring, 1, a : a + 1, cs], (SUB, LANE))
                if a != b:
                    second = jnp.broadcast_to(qb[ring, 1, b : b + 1, cs], (SUB, LANE))
                    v = jnp.where(sub < b * AGG - (t - 1) * SUB, v, second)
                got.append(v)
            return [got[0]] * tiles + [got[1]]

        def start_y(t):
            o = slice((t + 1) * SUB, (t + 2) * SUB)
            for c, v in enumerate(up(1, t)):
                y = st[SO, c, o] * v
                us[0, Y, c, o] = y
                us[0, Q, c, o] = y * y

        s_send.wait_recv()
        for t in range(1, bands - 1):
            start_y(t)

        e_send.wait_recv()
        start_y(0)
        start_y(bands - 1)
        for t in range(bands):
            o = slice((t + 1) * SUB, (t + 2) * SUB)
            for c, v in enumerate(up(0, t)):
                us[0, U, c, o] = st[HD, c, o] + st[EW, c, o] * v

        full = 1.0 / infiltration_rate

        def flows(q, o):
            h = [st[M2, c, o] * q[c] for c in range(width)]
            west, east = beside(h, h)
            return [
                jnp.maximum(east[c], 0.0) - jnp.minimum(west[c], 0.0) for c in range(width)
            ]

        def sums_u(u):
            west, east = beside(u, u)
            return [west[c] + east[c] for c in range(width)]

        def new_y(src, c, o, above, below, y, q, gu, side):
            return (
                (y + st[RI, c, o] * gu)
                + (st[M0, c, below] * us[src, Q, c, below] + st[M1, c, above] * us[src, Q, c, above])
                + (side - st[AD, c, o] * q)
            )

        def new_u(src, c, o, above, below, u, gu, side):
            total = (us[src, U, c, above] + us[src, U, c, below]) + side
            return (st[A1, c, o] * u - gu) + st[K, c, o] * total

        def held(src, k, o):
            return [us[src, k, c, o] for c in range(width)]

        def substep(src, dst):
            def band(t, carry):
                o, above, below = around(t)
                last = tiles - 1

                def get_u(c):
                    return us[src, U, c, o]

                def get_h(c):
                    return st[M2, c, o] * us[src, Q, c, o]

                ends = []
                for get in (get_u, get_h):
                    w_end, w_side = pltpu.roll(get(last), 1, 1), pltpu.roll(get(tiles), 1, 1)
                    e_end, e_side = (
                        pltpu.roll(get(0), LANE - 1, 1), pltpu.roll(get(tiles), LANE - 1, 1)
                    )
                    ends.append((w_end, w_side, e_end, e_side))
                first, final = lane == 0, lane == LANE - 1
                u, h = {}, {}
                for c in [*range(1, width), 0]:
                    for k in (c - 1, c, c + 1):
                        if k in range(width) and (c not in (0, tiles) or k == c) and k not in u:
                            u[k], h[k] = get_u(k), get_h(k)
                    west, east = [], []
                    for near, (w_end, w_side, e_end, e_side) in zip((u, h), ends):
                        if c == 0:
                            west.append(jnp.where(first, w_side, w_end))
                        elif c == tiles:
                            west.append(jnp.where(first, w_end, w_side))
                        else:
                            west.append(near[c - 1])
                        if c == last:
                            east.append(jnp.where(final, e_side, e_end))
                        elif c == tiles:
                            east.append(jnp.where(final, e_end, e_side))
                        else:
                            east.append(near[c + 1])
                    y = us[src, Y, c, o]
                    gu = u[c] * pl.reciprocal(y + full)
                    side = jnp.maximum(east[1], 0.0) - jnp.minimum(west[1], 0.0)
                    us[dst, U, c, o] = new_u(src, c, o, above, below, u[c], gu, west[0] + east[0])
                    y = new_y(src, c, o, above, below, y, us[src, Q, c, o], gu, side)
                    us[dst, Y, c, o] = y
                    us[dst, Q, c, o] = y * y
                return carry

            lax.fori_loop(0, bands, band, 0, unroll=UNROLL)

        def two(k, carry):
            substep(0, 1)
            substep(1, 0)
            return carry

        lax.fori_loop(0, NSUB // 2 - 1, two, 0)
        substep(0, 1)

        def last_y(t, carry):
            o, above, below = around(t)
            u, q = held(1, U, o), held(1, Q, o)
            q_sides = flows(q, o)
            total = None
            for c in range(tiles):
                y = us[1, Y, c, o]
                gu = u[c] * pl.reciprocal(y + full)
                y = new_y(1, c, o, above, below, y, q[c], gu, q_sides[c])
                total = y if total is None else total + y
            sums[0, pl.ds(aligned(t * SUB - SUB), SUB)] = total
            return carry

        def last_u(t, carry):
            o, above, below = around(t)
            u = held(1, U, o)
            u_sides = sums_u(u)
            total = None
            for c in range(tiles):
                gu = u[c] * pl.reciprocal(us[1, Y, c, o] + full)
                p = new_u(1, c, o, above, below, u[c], gu, u_sides[c]) * st[RI, c, o]
                total = p if total is None else total + p
            sums[1, pl.ds(aligned(t * SUB - SUB), SUB)] = total
            return carry

        lax.fori_loop(1, bands - 1, last_y, 0, unroll=True)
        back_tx[...] = pool(sums[0], infiltration_rate)
        back_send.start()
        lax.fori_loop(1, bands - 1, last_u, 0, unroll=True)
        out_ref[0] = pool(sums[1], infiltration_rate)
        over(range(4), lambda d: [c.wait_send() for c in route_sends(d)])
        corners(lambda d, s: corner_send(d, s).wait_send())
        back_send.wait_send()


UNROLL = 12


def per_device(ny, nx, column_water, land_soil, level_weight, excess_weight, soil_weight,
               terrain_class, surface_head, conductivity, active_mask, flow_code):
    rows, cols = terrain_class.shape
    lev = column_water.shape[1]
    crow, ccol = land_soil.shape[1:]
    wide = cols // LANE + 1
    tall = rows + 4 * SUB
    packs = -(-(rows // SUB) // 4)
    f32, i32, bf16 = jnp.float32, jnp.int32, jnp.bfloat16
    hbm = pl.BlockSpec(memory_space=pltpu.HBM)
    return pl.pallas_call(
        functools.partial(kernel, ny, nx),
        out_shape=pltpu.VMEM((1, crow, ccol), f32),
        in_specs=[hbm] * 10,
        out_specs=pl.BlockSpec(memory_space=pltpu.VMEM),
        scratch_shapes=[
            pltpu.SMEM(level_weight.shape, f32),
            pltpu.SMEM(excess_weight.shape, f32),
            pltpu.SMEM(soil_weight.shape, f32),
            pltpu.VMEM((2, rows, cols), i32),
            pltpu.VMEM((rows, cols), i32),
            pltpu.VMEM((2, rows, cols), f32),
            pltpu.VMEM((11, wide, tall, LANE), f32),
            pltpu.VMEM((2, 3, wide, tall, LANE), f32),
            pltpu.VMEM((lev, crow, ccol), f32),
            pltpu.VMEM((crow, ccol), f32),
            pltpu.VMEM((2, lev // 2, crow, ccol), f32),
            pltpu.VMEM((2, lev // 2, crow, ccol), f32),
            pltpu.VMEM((2, 2, crow, ccol), f32),
            pltpu.VMEM((8, 2, crow, ccol), f32),
            pltpu.VMEM((2, crow, ccol), f32),
            pltpu.VMEM((2, 2, crow, ccol), f32),
            pltpu.VMEM((2, 2, 2 * crow, 2 * ccol), f32),
            pltpu.VMEM((crow, ccol), f32),
            pltpu.VMEM((crow, ccol), f32),
            pltpu.VMEM((cols, ccol), bf16),
            pltpu.VMEM((cols, cols), bf16),
            pltpu.VMEM((PLANES * (rows - 2 * SUB), cols), bf16),
            pltpu.VMEM((2, FIELDS, wide - 1, SUB, LANE), f32),
            pltpu.VMEM((2, FIELDS, wide - 1, SUB, LANE), f32),
            pltpu.VMEM((2, rows, LANE), f32),
            pltpu.VMEM((2, packs, SUB, LANE), f32),
            pltpu.VMEM((2, packs, SUB, LANE), f32),
            pltpu.VMEM((2, 2, SUB, LANE), f32),
            pltpu.SemaphoreType.DMA((8, 3)),
            pltpu.SemaphoreType.DMA((8, 3)),
            pltpu.SemaphoreType.DMA((18,)),
            pltpu.SemaphoreType.DMA((6,)),
        ],
        compiler_params=pltpu.CompilerParams(
            collective_id=0, has_side_effects=True
        ),
    )(level_weight, excess_weight, soil_weight, column_water, land_soil, terrain_class,
      surface_head, conductivity, active_mask, flow_code)


def solution(mesh):
    in_specs = (
        P("comp", None, "gy", "gx"),
        P("comp", "gy", "gx"),
        P(),
        P(),
        P(),
        P("gy", "gx"),
        P("comp", "gy", "gx"),
        P("comp", "gy", "gx"),
        P("comp", "gy", "gx"),
        P("comp", "gy", "gx"),
    )
    body = functools.partial(per_device, mesh.shape["gy"], mesh.shape["gx"])
    return jax.shard_map(
        body, mesh=mesh, in_specs=in_specs, out_specs=P("comp", "gy", "gx"), check_vma=False
    )
```
